32 devices in a mesh: dp: 8 (over z, y), tensor: 4 (over x, core).
Axes of the slice: x: 2, y: 2, z: 4, core: 2. Of those that a mesh axis runs over, the one named last changes fastest.
Arguments:
- frames: bfloat16 [8192, 1024], P(('dp', 'tensor')), may hold values from -6 to 6
- cotangent: bfloat16 [8192, 1024], P(('dp', 'tensor')), may hold values from -6 to 6
- ada_gain: float32 [7, 2048], replicated, may hold values from 0.25 to 1.75
- ada_shift: float32 [7, 2048], replicated, may hold values from -4 to 4
- w_query: bfloat16 [1024, 1024], P(None, 'tensor'), may hold values from -0.25 to 0.25
- b_query: float32 [1024], P('tensor'), may hold values from -4 to 4
- w_key: bfloat16 [1024, 1024], P(None, 'tensor'), may hold values from -0.25 to 0.25
- w_value: bfloat16 [1024, 1024], P(None, 'tensor'), may hold values from -0.1875 to 0.1875
- b_value: float32 [1024], P('tensor'), may hold values from -4 to 4
- w_out: bfloat16 [1024, 1024], P('tensor'), may hold values from -1.5 to 1.5
- b_out: float32 [1024], replicated, may hold values from -4 to 4
- w_inner: bfloat16 [1024, 4096], P(None, 'tensor'), may hold values from -0.1875 to 0.1875
- b_inner: float32 [4096], P('tensor'), may hold values from -6 to 6
- w_outer: bfloat16 [4096, 1024], P('tensor'), may hold values from -0.09375 to 0.09375
- b_outer: float32 [1024], replicated, may hold values from -6 to 6
- section_index: int32 [8], P('dp'), may hold values from 2 to 8, as said below
- lengths: int32 [8], P('dp'), may hold values from 512 to 1024, as said below
- key_mask: int32 [8192], P('dp'), may hold values from 0 to 1, as said below
Outputs:
- layer_out: bfloat16 [8192, 1024], P(('dp', 'tensor'))
- frames_grad: float32 [8192, 1024], P(('dp', 'tensor'))
- grad_ada_gain: float32 [7, 2048], replicated
- grad_ada_shift: float32 [7, 2048], replicated
- grad_w_query: float32 [1024, 1024], P(None, 'tensor')
- grad_b_query: float32 [1024], P('tensor')
- grad_w_key: float32 [1024, 1024], P(None, 'tensor')
- grad_w_value: float32 [1024, 1024], P(None, 'tensor')
- grad_b_value: float32 [1024], P('tensor')
- grad_w_out: float32 [1024, 1024], P('tensor')
- grad_b_out: float32 [1024], replicated
- grad_w_inner: float32 [1024, 4096], P(None, 'tensor')
- grad_b_inner: float32 [4096], P('tensor')
- grad_w_outer: float32 [4096, 1024], P('tensor')
- grad_b_outer: float32 [1024], replicated
The draws below stay inside these ranges and needn't reach their ends.
Inputs may be any that keep to these rules, and one draw needn't show every extreme that they name: `section_index`: every one of the 7 sections is used by some sequence. `lengths`: some sequence has all 1024 frames. `key_mask`: the first frame of every sequence is 1.
All inputs are finite; a program needn't handle non-finite values.
Results may differ from the reference program's by a relative error of at most 0.015.
The reference program's roundings to bfloat16 on the way count: a program that leaves them out, or rounds other values in their place, can miss the bound.
Values may be sent and summed in bfloat16 or wider, within the bound.
A program may use at most 128 MiB of HBM per device.

```python
import jax
import jax.numpy as jnp
from jax import lax

D = 1024
HEADS = 16
HDIM = 64
FF = 4096
SECTIONS = 7
SEQ = 1024
SEQS = 8
TOKENS = 8192


def draw_section_index(key, part):
    earlier = jax.random.randint(jax.random.fold_in(key, 11), (SEQS,), 0, SECTIONS)
    later = jax.random.randint(jax.random.fold_in(key, 12), (SEQS,), 0, SECTIONS)
    skewed = jnp.minimum(earlier, later)
    ordering = jax.random.permutation(jax.random.fold_in(key, 13), SECTIONS).astype(jnp.int32)
    spread_out = jnp.concatenate([ordering, jnp.zeros((SEQS,), jnp.int32)])[:SEQS]
    position = jnp.arange(SEQS, dtype=jnp.int32)
    return (2 + jnp.where(position < SECTIONS, spread_out, skewed)).astype(jnp.int32)


def draw_lengths(key, part):
    values = jax.random.randint(jax.random.fold_in(key, 21), (SEQS,), SEQ // 2, SEQ + 1)
    chosen = jax.random.randint(jax.random.fold_in(key, 22), (), 0, SEQS)
    return jnp.where(jnp.arange(SEQS, dtype=jnp.int32) == chosen, SEQ, values).astype(jnp.int32)


def draw_key_mask(key, part):
    draws = jax.random.randint(jax.random.fold_in(key, 31), (TOKENS,), 0, 8)
    places = jnp.arange(TOKENS, dtype=jnp.int32) % SEQ
    return jnp.where((draws > 0) | (places == 0), 1, 0).astype(jnp.int32)


def shard_levels(key, extent, pieces, least, top_value):
    def one(axis_at, shards_of):
        heights = jax.random.uniform(jax.random.fold_in(jax.random.fold_in(key, 6), axis_at), (shards_of,), jnp.float32, least / len(pieces), top_value / len(pieces))
        return jnp.repeat(jnp.exp(heights), extent[axis_at] // shards_of).reshape((-1,) + (1,) * (len(extent) - axis_at - 1))

    loudness = one(*pieces[0])
    for cut in pieces[1:]:
        loudness = loudness * one(*cut)
    return loudness


def gaussian(own_key, dims, width, bound, cuts=(), kind=jnp.bfloat16):
    values = width * jax.random.normal(own_key, dims, jnp.float32)
    if cuts:
        values = values * shard_levels(own_key, dims, cuts, -0.22, 0.18)
    return jnp.clip(values, -bound, bound).astype(kind)


def setup_inputs(seed: int = 0) -> dict:
    arg_keys = jax.random.split(jax.random.key(seed), 19)
    return {
        "frames": gaussian(arg_keys[0], (TOKENS, D), 1.0, 6.0, ((0, 32),)),
        "cotangent": gaussian(arg_keys[1], (TOKENS, D), 1.0, 6.0, ((0, 32),)),
        "ada_gain": jnp.clip(1.0 + 0.15 * jax.random.normal(arg_keys[2], (SECTIONS, D * 2), jnp.float32), 0.25, 1.75),
        "ada_shift": gaussian(arg_keys[3], (SECTIONS, D * 2), 0.3, 4.0, (), jnp.float32),
        "w_query": gaussian(arg_keys[4], (D, D), (D // 2) ** -0.5, 0.25, ((1, 4),)),
        "b_query": gaussian(arg_keys[5], (D,), 0.3, 4.0, ((0, 4),), jnp.float32),
        "w_key": gaussian(arg_keys[6], (D, D), (D // 2) ** -0.5, 0.25, ((1, 4),)),
        "w_value": gaussian(arg_keys[7], (D, D), D ** -0.5, 0.1875, ((1, 4),)),
        "b_value": gaussian(arg_keys[8], (D,), 0.3, 4.0, ((0, 4),), jnp.float32),
        "w_out": gaussian(arg_keys[9], (D, D), (D // 64) ** -0.5, 1.5, ((0, 4),)),
        "b_out": gaussian(arg_keys[10], (D,), 0.3, 4.0, (), jnp.float32),
        "w_inner": gaussian(arg_keys[11], (D, FF), D ** -0.5, 0.1875, ((1, 4),)),
        "b_inner": gaussian(arg_keys[12], (FF,), 0.5, 6.0, ((0, 4),), jnp.float32),
        "w_outer": gaussian(arg_keys[13], (FF, D), FF ** -0.5, 0.09375, ((0, 4),)),
        "b_outer": gaussian(arg_keys[14], (D,), 0.5, 6.0, (), jnp.float32),
        "section_index": draw_section_index(jax.random.fold_in(arg_keys[18], 71), 0),
        "lengths": draw_lengths(jax.random.fold_in(arg_keys[18], 71), 0),
        "key_mask": draw_key_mask(jax.random.fold_in(arg_keys[18], 71), 0),
    }


EPSILON = 1e-05
NEG_LARGE = -1e+30
PRECISE = lax.Precision.HIGHEST

@jax.custom_vjp
def low(v):
    return lax.optimization_barrier(v.astype(jnp.bfloat16)).astype(jnp.float32)

@jax.custom_vjp
def low_back(v):
    return v

def low_keep(v):
    return (low(v), None)

def low_pass(kept, grad):
    return (grad,)

def back_keep(v):
    return (v, None)

def back_low(kept, grad):
    return (low(grad),)
low.defvjp(low_keep, low_pass)
low_back.defvjp(back_keep, back_low)

def normalize(row_block):
    centered = row_block - lax.optimization_barrier(jnp.mean(row_block, axis=-1, keepdims=True))
    return centered * lax.rsqrt(lax.optimization_barrier(jnp.mean(centered * centered, axis=-1, keepdims=True)) + EPSILON)

def matmul(left_side, right_side):
    return jnp.dot(left_side, right_side, preferred_element_type=jnp.float32, precision=PRECISE)

def heads_of(flat_rows):
    return flat_rows.reshape(SEQ, HEADS, HDIM)

def attend_sequence(packed):
    queries, keys_all, values_all, valid_keys = packed
    scores = jnp.einsum('qhe,khe->hqk', heads_of(queries), heads_of(keys_all), precision=PRECISE) * HDIM ** (-0.5)
    scores = jnp.where(valid_keys[None, None, :], low_back(scores), NEG_LARGE)
    softmax_low = low(jax.nn.softmax(scores, axis=-1))
    mixture = jnp.einsum('hqk,khe->qhe', softmax_low, heads_of(values_all), precision=PRECISE)
    return low(low_back(mixture.reshape(SEQ, D)))

def forward(frames, ada_gain, ada_shift, w_query, b_query, w_key, w_value, b_value, w_out, b_out, w_inner, b_inner, w_outer, b_outer, section_index, lengths, key_mask):
    onehot = (section_index[:, None] - 2 == jnp.arange(SECTIONS, dtype=jnp.int32)[None, :]).astype(jnp.float32)
    seq_gain = matmul(onehot, ada_gain)[:, None, :]
    seq_shift = matmul(onehot, ada_shift)[:, None, :]
    places = jnp.arange(SEQ, dtype=jnp.int32)
    valid_keys = (places[None, :] < lengths[:, None]) & (key_mask.reshape(SEQS, SEQ) > 0)
    first_norm = low(normalize(frames.reshape(SEQS, SEQ, D)) * seq_gain[..., :D] + seq_shift[..., :D]).reshape(TOKENS, D)
    queries = low(low_back(matmul(first_norm, w_query) + b_query))
    keys_all = low(low_back(matmul(first_norm, w_key)))
    values_all = low(low_back(matmul(first_norm, w_value) + b_value))
    attended = lax.map(jax.checkpoint(attend_sequence), (queries.reshape(SEQS, SEQ, D), keys_all.reshape(SEQS, SEQ, D), values_all.reshape(SEQS, SEQ, D), valid_keys)).reshape(TOKENS, D)
    hidden = frames + low_back(matmul(attended, w_out)) + b_out
    second_norm = low(normalize(hidden.reshape(SEQS, SEQ, D)) * seq_gain[..., D:] + seq_shift[..., D:]).reshape(TOKENS, D)
    inner_pre = low_back(matmul(second_norm, w_inner) + b_inner)
    activated = low(jax.nn.gelu(inner_pre, approximate=False))
    return hidden + matmul(activated, w_outer) + b_outer

def reference(frames, cotangent, ada_gain, ada_shift, w_query, b_query, w_key, w_value, b_value, w_out, b_out, w_inner, b_inner, w_outer, b_outer, section_index, lengths, key_mask):
    floats = tuple((member.astype(jnp.float32) for member in (frames, ada_gain, ada_shift, w_query, b_query, w_key, w_value, b_value, w_out, b_out, w_inner, b_inner, w_outer, b_outer)))

    def bound_forward(*params):
        return forward(*params, section_index, lengths, key_mask)
    result, pullback = jax.vjp(bound_forward, *floats)
    gradients = pullback(cotangent.astype(jnp.float32))
    return (result.astype(jnp.bfloat16), gradients[0], gradients[1], gradients[2], gradients[3], gradients[4], gradients[5], gradients[6], gradients[7], gradients[8], gradients[9], gradients[10], gradients[11], gradients[12], gradients[13])
```

```python
import functools

import jax
import jax.numpy as jnp
from jax import lax
from jax.experimental import pallas as pl
from jax.experimental.pallas import tpu as pltpu
from jax.sharding import PartitionSpec as P

HDIM = 64
SEQ = 1024
EPSILON = 1e-05
NEG_LARGE = -1e30
F32 = jnp.float32
BF16 = jnp.bfloat16
MESH = pl.DeviceIdType.MESH
VMEM_LIMIT = 60 * 1024 * 1024


def places():
    dp = lax.axis_index("dp")
    me = lax.axis_index("tensor")
    sib = me + 1 - 2 * (me % 2)
    across = (me + 2) % 4
    diag = (sib + 2) % 4
    return dp, me, sib, across, diag


def greet(partners):
    barrier = pltpu.get_barrier_semaphore()
    for partner in partners:
        pl.semaphore_signal(barrier, inc=1, device_id=partner, device_id_type=MESH)
    pl.semaphore_wait(barrier, len(partners))


def remote(src, dst, send, recv, device):
    return pltpu.make_async_remote_copy(
        src_ref=src, dst_ref=dst, send_sem=send, recv_sem=recv, device_id=device, device_id_type=MESH
    )


def whole_vmem(count):
    return [pl.BlockSpec(memory_space=pltpu.VMEM)] * count


PARTS = 4


def gather_kernel(x_ref, o_ref, send, recv):
    dp, me, sib, across, diag = places()
    rows = x_ref.shape[0]
    part = rows // PARTS
    greet([(dp, sib), (dp, across)])
    copies = []
    for i in range(PARTS):
        at = pl.multiple_of(me * rows + i * part, part)
        copies.append(
            remote(x_ref.at[pl.ds(i * part, part)], o_ref.at[pl.ds(at, part)], send.at[i], recv.at[i], (dp, across))
        )
        copies[-1].start()
    mine = pl.ds(pl.multiple_of(me * rows, rows), rows)
    copies.append(remote(x_ref, o_ref.at[mine], send.at[PARTS], recv.at[PARTS], (dp, sib)))
    copies[-1].start()
    o_ref[mine, :] = x_ref[...]
    for i in range(PARTS):
        copies[i].wait_recv()
        there = pl.ds(pl.multiple_of(across * rows + i * part, part), part)
        j = PARTS + 1 + i
        copies.append(remote(o_ref.at[there], o_ref.at[there], send.at[j], recv.at[j], (dp, sib)))
        copies[-1].start()
    for i, copy in enumerate(copies):
        if i >= PARTS:
            copy.wait_recv()
        copy.wait_send()


def tensor_gather(block, cid):
    rows, width = block.shape
    return pl.pallas_call(
        gather_kernel,
        out_shape=jax.ShapeDtypeStruct((rows * 4, width), block.dtype),
        in_specs=whole_vmem(1),
        out_specs=pl.BlockSpec(memory_space=pltpu.VMEM),
        scratch_shapes=[pltpu.SemaphoreType.DMA((2 * PARTS + 1,))] * 2,
        compiler_params=pltpu.CompilerParams(collective_id=cid, has_side_effects=True, vmem_limit_bytes=VMEM_LIMIT),
        name="tensor_gather_%d" % cid,
    )(block)


def scatter_kernel(p_ref, o_ref, from_sib, chip_sum, landed, send, recv):
    dp, me, sib, across, diag = places()
    rows = p_ref.shape[0] // 4
    part = rows // PARTS
    greet([(dp, sib), (dp, across)])

    def at(owner, i):
        return pl.ds(pl.multiple_of(owner * rows + i * part, part), part)

    first, last = [], []
    for i in range(PARTS):
        here = pl.ds(i * part, part)
        first.append(remote(p_ref.at[at(diag, i)], from_sib.at[0, here], send.at[i], recv.at[i], (dp, sib)))
        first[-1].start()
    for i in range(PARTS):
        here = pl.ds(i * part, part)
        j = PARTS + i
        last.append(remote(p_ref.at[at(sib, i)], from_sib.at[1, here], send.at[j], recv.at[j], (dp, sib)))
        last[-1].start()
    crossing = []
    for i in range(PARTS):
        here = pl.ds(i * part, part)
        j = 2 * PARTS + i
        first[i].wait_recv()
        chip_sum[here, :] = (p_ref[at(across, i), :].astype(F32) + from_sib[0, here, :].astype(F32)).astype(BF16)
        crossing.append(remote(chip_sum.at[here], landed.at[here], send.at[j], recv.at[j], (dp, across)))
        crossing[-1].start()
    for i in range(PARTS):
        here = pl.ds(i * part, part)
        last[i].wait_recv()
        o_ref[here, :] = p_ref[at(me, i), :].astype(F32) + from_sib[1, here, :].astype(F32)
    for i in range(PARTS):
        here = pl.ds(i * part, part)
        crossing[i].wait_recv()
        o_ref[here, :] = o_ref[here, :] + landed[here, :].astype(F32)
    for copy in first + last + crossing:
        copy.wait_send()


def tensor_scatter(partial, cid):
    rows, width = partial.shape[0] // 4, partial.shape[1]
    return pl.pallas_call(
        scatter_kernel,
        out_shape=jax.ShapeDtypeStruct((rows, width), F32),
        in_specs=whole_vmem(1),
        out_specs=pl.BlockSpec(memory_space=pltpu.VMEM),
        scratch_shapes=[
            pltpu.VMEM((2, rows, width), BF16),
            pltpu.VMEM((rows, width), BF16),
            pltpu.VMEM((rows, width), BF16),
            pltpu.SemaphoreType.DMA((3 * PARTS,)),
            pltpu.SemaphoreType.DMA((3 * PARTS,)),
        ],
        compiler_params=pltpu.CompilerParams(collective_id=cid, has_side_effects=True, vmem_limit_bytes=VMEM_LIMIT),
        name="tensor_scatter_%d" % cid,
    )(partial)


def dp_lines(count):
    sizes, limit = [], 2
    while count > 1:
        size = min(count, limit)
        sizes.append(size)
        count //= size
        limit *= 2
    return sizes


class Line:
    def __init__(self, size, stride, dp, me):
        self.size = size
        self.place = (dp // stride) % size
        self.right = (jnp.minimum(dp + stride, dp + (size - 1 - self.place) * stride), me)
        self.left = (jnp.maximum(dp - stride, dp - self.place * stride), me)
        self.pair = (dp + stride - 2 * stride * (dp // stride % 2), me)


def lines_of(count, dp, me):
    found, stride = [], 1
    for size in dp_lines(count):
        found.append(Line(size, stride, dp, me))
        stride *= size
    return found


def chunk_sems(count):
    sizes = dp_lines(count)
    return 1 + sizes[1] + sum(4 * size for size in sizes[1:])


def chunk_scratch(count, rows, width):
    sizes = dp_lines(count)
    shapes = [pltpu.VMEM((rows // 2, width), BF16), pltpu.VMEM((rows // 2, width), BF16)]
    part = rows // 2
    for size in sizes[1:]:
        part //= size
        shapes += [pltpu.VMEM((size, part, width), BF16)] * 2
    return shapes


def sum_chunk(lines, x_ref, o_ref, columns, scratch, send, recv):
    rows = x_ref.shape[0]
    got, own = scratch[0], scratch[1]
    buffers = [scratch[2 + 2 * i : 4 + 2 * i] for i in range(len(lines) - 1)]
    pair = lines[0]
    half = rows // 2
    started = []
    used = [0]

    def slots(count):
        used[0] += count
        return used[0] - count

    def go(copy, condition=None):
        if condition is None:
            copy.start()
        else:
            pl.when(condition)(lambda: copy.start())
        started.append((copy, condition))

    def when(condition, body):
        pl.when(condition)(body)

    mine = pl.multiple_of(pair.place * half, half)
    other = pl.multiple_of(half - pair.place * half, half)
    slot = slots(1)
    first = remote(x_ref.at[pl.ds(other, half), columns], got, send.at[slot], recv.at[slot], pair.pair)
    go(first)
    yield
    first.wait_recv()
    own[...] = (x_ref[pl.ds(mine, half), columns].astype(F32) + got[...].astype(F32)).astype(BF16)
    base = 0
    size_now = half
    for line, (to_right, to_left) in zip(lines[1:], buffers):
        n, z = line.size, line.place
        part = size_now // n
        right_slot, left_slot = slots(n), slots(n)
        bases = base

        def piece(o, part=part, bases=bases):
            return pl.ds(pl.multiple_of(bases + o * part, part), part)

        for j in range(n - 1, 0, -1):
            for way in (0, 1):
                o = z + j if way == 0 else z - j
                inside = (o < n) if way == 0 else (o >= 0)
                buffer = to_right if way == 0 else to_left
                at_end = (z == 0) if way == 0 else (z == n - 1)
                slot = (right_slot if way == 0 else left_slot) + jnp.clip(o, 0, n - 1)
                o = jnp.clip(o, 0, n - 1)
                there = line.right if way == 0 else line.left
                copy = remote(own.at[piece(o)], buffer.at[o], send.at[slot], recv.at[slot], there)
                onward = remote(buffer.at[o], buffer.at[o], send.at[slot], recv.at[slot], there)
                go(copy, inside & at_end)

                def pass_on(buffer=buffer, o=o, onward=onward, piece=piece):
                    onward.wait_recv()
                    buffer[o] = (buffer[o].astype(F32) + own[piece(o), :].astype(F32)).astype(BF16)
                    onward.start()

                when(inside & jnp.logical_not(at_end), pass_on)
                started.append((onward, inside & jnp.logical_not(at_end)))
            yield

        def take(buffer, slot, line=line, piece=piece, z=z):
            remote(buffer.at[z], buffer.at[z], send.at[slot + z], recv.at[slot + z], line.right).wait_recv()
            own[piece(z), :] = (own[piece(z), :].astype(F32) + buffer[z].astype(F32)).astype(BF16)

        when(z > 0, functools.partial(take, to_right, right_slot))
        when(z < n - 1, functools.partial(take, to_left, left_slot))
        base = bases + z * part
        size_now = part
    final = pl.ds(pl.multiple_of(mine + base, size_now), size_now)
    o_ref[final, columns] = own[pl.ds(pl.multiple_of(base, size_now), size_now), :]
    region = mine + base
    for level in range(len(lines) - 1, 0, -1):
        line = lines[level]
        n, z = line.size, line.place
        part = size_now
        base_region = region - z * part
        right_slot, left_slot = slots(n), slots(n)
        pair_slot = slots(n) if level == 1 else None

        def piece(o, part=part, base_region=base_region):
            return pl.ds(pl.multiple_of(base_region + o * part, part), part)

        def copy_of(o, slot, there, piece=piece):
            ref = o_ref.at[piece(o), columns]
            return remote(ref, ref, send.at[slot + o], recv.at[slot + o], there)

        go(copy_of(z, right_slot, line.right), z < n - 1)
        go(copy_of(z, left_slot, line.left), z > 0)
        if level == 1:
            go(copy_of(z, pair_slot, pair.pair))
        yield
        for j in range(1, n):
            for way in (0, 1):
                o = z - j if way == 0 else z + j
                inside = (o >= 0) if way == 0 else (o < n)
                goes_on = (z < n - 1) if way == 0 else (z > 0)
                o = jnp.clip(o, 0, n - 1)
                slot = right_slot if way == 0 else left_slot
                there = line.right if way == 0 else line.left
                copy = copy_of(o, slot, there)
                when(inside, lambda copy=copy: copy.wait_recv())
                go(copy, inside & goes_on)
                if level == 1:
                    go(copy_of(o, pair_slot, pair.pair), inside)
            yield
        region = base_region
        size_now = part * n
        if level == 1:
            for o in range(n):
                ref = o_ref.at[pl.ds(pl.multiple_of(other + o * part, part), part), columns]
                remote(ref, ref, send.at[pair_slot + o], recv.at[pair_slot + o], pair.pair).wait_recv()
    for copy, condition in started:
        if condition is None:
            copy.wait_send()
        else:
            when(condition, lambda copy=copy: copy.wait_send())


def run_skewed(makers):
    makers = list(makers)
    running = []
    while makers or running:
        if makers:
            running.append(makers.pop(0)())
        still = []
        for generator in running:
            try:
                next(generator)
                still.append(generator)
            except StopIteration:
                pass
        running = still


def dp_sum_kernel(count, widths, *refs):
    arrays = len(widths)
    ins, rest = refs[:arrays], refs[arrays:]
    vec_ref, bias_ref, pick_ref = rest[:3]
    outs, rest = rest[3 : 3 + arrays], rest[3 + arrays :]
    small_out, rest = rest[0], rest[1:]
    small_in, vec_got, vec_send, vec_recv = rest[:4]
    rest = rest[4:]
    dp, me, sib, across, diag = places()
    lines = lines_of(count, dp, me)
    others = [lines[0].pair]
    near = [(dp, sib), (dp, across), (dp, diag)]
    barrier = pltpu.get_barrier_semaphore()
    for partner in near + others:
        pl.semaphore_signal(barrier, inc=1, device_id=partner, device_id_type=MESH)
    waits = len(near) + len(others)
    for line in lines[1:]:
        has_right = line.place < line.size - 1
        has_left = line.place > 0
        for partner, has in ((line.right, has_right), (line.left, has_left)):
            pl.when(has)(
                lambda partner=partner: pl.semaphore_signal(
                    barrier, inc=1, device_id=partner, device_id_type=MESH
                )
            )
        waits = waits + has_right.astype(jnp.int32) + has_left.astype(jnp.int32)
    pl.semaphore_wait(barrier, waits)
    vec_copies = []
    for i, device in enumerate(near):
        vec_copies.append(remote(vec_ref, vec_got.at[i], vec_send.at[i], vec_recv.at[i], device))
        vec_copies[-1].start()

    per = 2 + 2 * (len(lines) - 1)
    makers = []
    for array in range(arrays):
        wide = ins[array].shape[1]
        for start in range(0, wide, widths[array]):
            scratch, rest = rest[:per], rest[per:]
            send, recv = rest[:2]
            rest = rest[2:]
            makers.append(
                functools.partial(
                    sum_chunk, lines, ins[array], outs[array], pl.ds(start, widths[array]), scratch, send, recv
                )
            )

    def small():
        for copy in vec_copies:
            copy.wait_recv()
        total = vec_ref[...] + vec_got[0] + vec_got[1] + vec_got[2]
        sections = pick_ref.shape[0]
        for s in range(sections):
            small_in[pl.ds(32 * s, 32), :] = (total[0:32] * pick_ref[s : s + 1, :]).astype(BF16)
        small_in[pl.ds(32 * sections, 16), :] = total[32:48].astype(BF16)
        small_in[pl.ds(32 * sections + 16, 16), :] = bias_ref[...].astype(BF16)
        done = 32 * sections + 32
        if done < small_in.shape[0]:
            small_in[pl.ds(done, small_in.shape[0] - done), :] = jnp.zeros((small_in.shape[0] - done, 128), BF16)
        yield from sum_chunk(lines, small_in, small_out, slice(None), rest[:per], rest[per], rest[per + 1])

    run_skewed(makers + [small])
    for copy in vec_copies:
        copy.wait_send()


def dp_sum(count, grads, widths, vec, bias, pick, cid):
    small_rows = max(16 * count, -(-(32 * pick.shape[0] + 32) // (16 * count)) * 16 * count)
    sems = chunk_sems(count)
    scratch = [
        pltpu.VMEM((small_rows, 128), BF16),
        pltpu.VMEM((3,) + vec.shape, F32),
        pltpu.SemaphoreType.DMA((3,)),
        pltpu.SemaphoreType.DMA((3,)),
    ]
    for grad, width in zip(grads, widths):
        for _ in range(0, grad.shape[1], width):
            scratch += chunk_scratch(count, grad.shape[0], width)
            scratch += [pltpu.SemaphoreType.DMA((sems,))] * 2
    scratch += chunk_scratch(count, small_rows, 128)
    scratch += [pltpu.SemaphoreType.DMA((sems,))] * 2
    return pl.pallas_call(
        functools.partial(dp_sum_kernel, count, tuple(widths)),
        out_shape=[jax.ShapeDtypeStruct(g.shape, BF16) for g in grads]
        + [jax.ShapeDtypeStruct((small_rows, 128), BF16)],
        in_specs=whole_vmem(len(grads) + 3),
        out_specs=whole_vmem(len(grads) + 1),
        scratch_shapes=scratch,
        compiler_params=pltpu.CompilerParams(collective_id=cid, has_side_effects=True, vmem_limit_bytes=VMEM_LIMIT),
        name="dp_sum",
    )(*grads, vec, bias, pick)


def normalize(row_block):
    centered = row_block - jnp.mean(row_block, axis=-1, keepdims=True)
    inverse = lax.rsqrt(jnp.mean(centered * centered, axis=-1, keepdims=True) + EPSILON)
    return (centered * inverse, inverse)


def norm_back(grad_hat, normed, inverse):
    return inverse * (
        grad_hat
        - jnp.mean(grad_hat, axis=-1, keepdims=True)
        - normed * jnp.mean(grad_hat * normed, axis=-1, keepdims=True)
    )


def exact_gelu(values):
    return jax.nn.gelu(values, approximate=False)


def split_heads(flat_rows):
    return flat_rows.reshape(-1, SEQ, flat_rows.shape[1] // HDIM, HDIM)


def dot(a, b, dims):
    return lax.dot_general(a, b, (dims, ((), ())), preferred_element_type=F32)


def masked_scores(query_block, keys_all, valid_keys, score_scale):
    scores = jnp.einsum("sqhe,skhe->shqk", query_block, keys_all, preferred_element_type=F32) * score_scale
    return jnp.where(valid_keys[:, None, None, :], scores, NEG_LARGE)


def attention_forward(queries, keys_all, values_all, valid_keys, score_scale, block_rows):
    pieces = []
    log_sums = []
    for offset in range(0, SEQ, block_rows):
        scores = masked_scores(queries[:, offset : offset + block_rows], keys_all, valid_keys, score_scale)
        highest = jnp.max(scores, axis=-1, keepdims=True)
        weights = jnp.exp(scores - highest)
        totals = jnp.sum(weights, axis=-1, keepdims=True)
        softmax_low = (weights / totals).astype(BF16)
        mixture = jnp.einsum("shqk,skhe->sqhe", softmax_low, values_all, preferred_element_type=F32)
        pieces.append(mixture.astype(BF16))
        log_sums.append((highest + jnp.log(totals))[..., 0])
    return (jnp.concatenate(pieces, axis=1), jnp.concatenate(log_sums, axis=2))


def attention_backward(queries, keys_all, values_all, grad_attended, log_sums, valid_keys, score_scale, block_rows):
    grad_keys = jnp.zeros(keys_all.shape, F32)
    grad_values = jnp.zeros(values_all.shape, F32)
    grad_pieces = []
    for offset in range(0, SEQ, block_rows):
        query_block = queries[:, offset : offset + block_rows]
        grad_block = grad_attended[:, offset : offset + block_rows]
        scores = masked_scores(query_block, keys_all, valid_keys, score_scale)
        softmax_rows = jnp.exp(scores - log_sums[:, :, offset : offset + block_rows, None])
        grad_probs = jnp.einsum("sqhe,skhe->shqk", grad_block, values_all, preferred_element_type=F32)
        centre = jnp.sum(softmax_rows * grad_probs, axis=-1, keepdims=True)
        grad_scores = (softmax_rows * (grad_probs - centre)).astype(BF16)
        grad_pieces.append(
            jnp.einsum("shqk,skhe->sqhe", grad_scores, keys_all, preferred_element_type=F32) * score_scale
        )
        grad_keys = (
            grad_keys + jnp.einsum("shqk,sqhe->skhe", grad_scores, query_block, preferred_element_type=F32) * score_scale
        )
        grad_values = grad_values + jnp.einsum(
            "shqk,sqhe->skhe", softmax_rows.astype(BF16), grad_block, preferred_element_type=F32
        )
    return (jnp.concatenate(grad_pieces, axis=1), grad_keys, grad_values)


def body(
    dp_count,
    frames,
    cotangent,
    ada_gain,
    ada_shift,
    w_query,
    b_query,
    w_key,
    w_value,
    b_value,
    w_out,
    b_out,
    w_inner,
    b_inner,
    w_outer,
    b_outer,
    section_index,
    lengths,
    key_mask,
):
    rows_dev, width = frames.shape
    sections = ada_gain.shape[0]
    assert section_index.shape[0] == 1
    score_scale = HDIM ** (-0.5)
    block_rows = 512
    section = section_index[0] - 2
    gain = lax.dynamic_slice(ada_gain, (section, 0), (1, 2 * width))
    shift = lax.dynamic_slice(ada_shift, (section, 0), (1, 2 * width))
    pick = jnp.broadcast_to(
        (section == jnp.arange(sections, dtype=jnp.int32)).astype(F32)[:, None], (sections, 128)
    )
    spots = jnp.arange(SEQ, dtype=jnp.int32)
    valid_keys = (spots[None, :] < lengths[:, None]) & (key_mask.reshape(1, SEQ) > 0)
    inputs = frames.astype(F32)
    normed_one, inverse_one = normalize(inputs)
    first_low = (normed_one * gain[:, :width] + shift[:, :width]).astype(BF16)
    first_all = tensor_gather(first_low, 1)
    queries = (dot(first_all, w_query, ((1,), (0,))) + b_query).astype(BF16)
    keys_all = dot(first_all, w_key, ((1,), (0,))).astype(BF16)
    values_all = (dot(first_all, w_value, ((1,), (0,))) + b_value).astype(BF16)
    attended_heads, log_sums = attention_forward(
        split_heads(queries), split_heads(keys_all), split_heads(values_all), valid_keys, score_scale, block_rows
    )
    attended = attended_heads.reshape(queries.shape)
    hidden = inputs + tensor_scatter(dot(attended, w_out, ((1,), (0,))).astype(BF16), 2) + b_out
    normed_two, inverse_two = normalize(hidden)
    second_low = (normed_two * gain[:, width:] + shift[:, width:]).astype(BF16)
    second_all = tensor_gather(second_low, 3)
    grad_all = tensor_gather(cotangent, 4)
    inner_pre = dot(second_all, w_inner, ((1,), (0,))) + b_inner
    activated = exact_gelu(inner_pre).astype(BF16)
    layer_out = (
        hidden + tensor_scatter(dot(activated, w_outer, ((1,), (0,))).astype(BF16), 5) + b_outer
    ).astype(BF16)
    grad_w_outer = dot(activated, grad_all, ((0,), (0,))).astype(BF16)
    grad_activated = dot(grad_all, w_outer, ((1,), (1,)))
    unused_value, gelu_pull = jax.vjp(exact_gelu, inner_pre)
    grad_inner = gelu_pull(grad_activated)[0].astype(BF16)
    grad_w_inner = dot(second_all, grad_inner, ((0,), (0,))).astype(BF16)
    grad_b_inner = jnp.sum(grad_inner.astype(F32), axis=0)
    grad_second = tensor_scatter(dot(grad_inner, w_inner, ((1,), (1,))).astype(BF16), 6)
    grad_out_rows = cotangent.astype(F32)
    grad_hidden = grad_out_rows + norm_back(grad_second * gain[:, width:], normed_two, inverse_two)
    grad_attn_all = tensor_gather(grad_hidden.astype(BF16), 7)
    grad_w_out = dot(grad_attn_all, attended, ((0,), (0,)))
    grad_attended = dot(grad_attn_all, w_out, ((1,), (1,))).astype(BF16)
    grad_q_heads, grad_k_heads, grad_v_heads = attention_backward(
        split_heads(queries),
        split_heads(keys_all),
        split_heads(values_all),
        split_heads(grad_attended),
        log_sums,
        valid_keys,
        score_scale,
        block_rows,
    )
    grad_queries = grad_q_heads.reshape(queries.shape).astype(BF16)
    grad_keys = grad_k_heads.reshape(queries.shape).astype(BF16)
    grad_values = grad_v_heads.reshape(queries.shape).astype(BF16)
    grad_b_query = jnp.sum(grad_queries.astype(F32), axis=0)
    grad_b_value = jnp.sum(grad_values.astype(F32), axis=0)
    total_rows = dot(grad_queries, w_query, ((1,), (1,)))
    total_rows = total_rows + dot(grad_keys, w_key, ((1,), (1,)))
    total_rows = total_rows + dot(grad_values, w_value, ((1,), (1,)))
    grad_first = tensor_scatter(total_rows.astype(BF16), 8)
    grad_w_attn = jnp.concatenate(
        [
            dot(first_all, grad_queries, ((0,), (0,))).astype(BF16),
            dot(first_all, grad_keys, ((0,), (0,))).astype(BF16),
            dot(first_all, grad_values, ((0,), (0,))).astype(BF16),
            grad_w_out.astype(BF16),
        ],
        axis=1,
    )
    frames_grad = grad_hidden + norm_back(grad_first * gain[:, :width], normed_one, inverse_one)
    vec = jnp.concatenate(
        [
            jnp.sum(grad_first * normed_one, axis=0),
            jnp.sum(grad_second * normed_two, axis=0),
            jnp.sum(grad_first, axis=0),
            jnp.sum(grad_second, axis=0),
            jnp.sum(grad_hidden, axis=0),
            jnp.sum(grad_out_rows, axis=0),
        ]
    ).reshape(-1, 128)
    bias = jnp.concatenate(
        [grad_b_inner, grad_b_query, grad_b_value, jnp.zeros((2048 - 1024 - 512,), F32)]
    ).reshape(16, 128)
    sum_inner, sum_outer, sum_attn, small = dp_sum(
        dp_count, [grad_w_inner, grad_w_outer, grad_w_attn], [512, 512, 512], vec, bias, pick, 9
    )
    small = small.astype(F32)
    tables = small[: 32 * sections].reshape(sections, 2, 2 * width)
    shared = small[32 * sections : 32 * sections + 16].reshape(2, width)
    biases = small[32 * sections + 16 : 32 * sections + 32].reshape(-1)
    heads = w_query.shape[1]
    units = w_inner.shape[1]
    return (
        layer_out,
        frames_grad,
        tables[:, 0],
        tables[:, 1],
        sum_attn[:, :heads].astype(F32),
        biases[units : units + heads],
        sum_attn[:, heads : 2 * heads].astype(F32),
        sum_attn[:, 2 * heads : 3 * heads].astype(F32),
        biases[units + heads : units + 2 * heads],
        sum_attn[:, 3 * heads :].T.astype(F32),
        shared[0],
        sum_inner.astype(F32),
        biases[:units],
        sum_outer.astype(F32),
        shared[1],
    )


def solution(mesh):
    return jax.shard_map(
        functools.partial(body, mesh.shape["dp"]),
        mesh=mesh,
        in_specs=(
            P(("dp", "tensor"), None),
            P(("dp", "tensor"), None),
            P(),
            P(),
            P(None, "tensor"),
            P("tensor"),
            P(None, "tensor"),
            P(None, "tensor"),
            P("tensor"),
            P("tensor", None),
            P(),
            P(None, "tensor"),
            P("tensor"),
            P("tensor", None),
            P(),
            P("dp"),
            P("dp"),
            P("dp"),
        ),
        out_specs=(
            P(("dp", "tensor"), None),
            P(("dp", "tensor"), None),
            P(),
            P(),
            P(None, "tensor"),
            P("tensor"),
            P(None, "tensor"),
            P(None, "tensor"),
            P("tensor"),
            P("tensor", None),
            P(),
            P(None, "tensor"),
            P("tensor"),
            P("tensor", None),
            P(),
        ),
        check_vma=False,
    )
```

```python
import functools

import jax
import jax.numpy as jnp
from jax import lax
from jax.experimental import pallas as pl
from jax.experimental.pallas import tpu as pltpu
from jax.sharding import PartitionSpec as P

HDIM = 64
SEQ = 1024
EPSILON = 1e-05
NEG_LARGE = -1e30
F32 = jnp.float32
BF16 = jnp.bfloat16
MESH = pl.DeviceIdType.MESH
VMEM_LIMIT = 60 * 1024 * 1024


def places():
    dp = lax.axis_index("dp")
    me = lax.axis_index("tensor")
    sib = me + 1 - 2 * (me % 2)
    across = (me + 2) % 4
    diag = (sib + 2) % 4
    return dp, me, sib, across, diag


def greet(partners):
    barrier = pltpu.get_barrier_semaphore()
    for partner in partners:
        pl.semaphore_signal(barrier, inc=1, device_id=partner, device_id_type=MESH)
    pl.semaphore_wait(barrier, len(partners))


def remote(src, dst, send, recv, device):
    return pltpu.make_async_remote_copy(
        src_ref=src, dst_ref=dst, send_sem=send, recv_sem=recv, device_id=device, device_id_type=MESH
    )


def whole_vmem(count):
    return [pl.BlockSpec(memory_space=pltpu.VMEM)] * count


PARTS = 4


def gather_kernel(x_ref, o_ref, send, recv):
    dp, me, sib, across, diag = places()
    rows = x_ref.shape[0]
    part = rows // PARTS
    greet([(dp, sib), (dp, across)])
    copies = []
    for i in range(PARTS):
        at = pl.multiple_of(me * rows + i * part, part)
        copies.append(
            remote(x_ref.at[pl.ds(i * part, part)], o_ref.at[pl.ds(at, part)], send.at[i], recv.at[i], (dp, across))
        )
        copies[-1].start()
    mine = pl.ds(pl.multiple_of(me * rows, rows), rows)
    copies.append(remote(x_ref, o_ref.at[mine], send.at[PARTS], recv.at[PARTS], (dp, sib)))
    copies[-1].start()
    o_ref[mine, :] = x_ref[...]
    for i in range(PARTS):
        copies[i].wait_recv()
        there = pl.ds(pl.multiple_of(across * rows + i * part, part), part)
        j = PARTS + 1 + i
        copies.append(remote(o_ref.at[there], o_ref.at[there], send.at[j], recv.at[j], (dp, sib)))
        copies[-1].start()
    for i, copy in enumerate(copies):
        if i >= PARTS:
            copy.wait_recv()
        copy.wait_send()


def tensor_gather(block, cid):
    rows, width = block.shape
    return pl.pallas_call(
        gather_kernel,
        out_shape=jax.ShapeDtypeStruct((rows * 4, width), block.dtype),
        in_specs=whole_vmem(1),
        out_specs=pl.BlockSpec(memory_space=pltpu.VMEM),
        scratch_shapes=[pltpu.SemaphoreType.DMA((2 * PARTS + 1,))] * 2,
        compiler_params=pltpu.CompilerParams(collective_id=cid, has_side_effects=True, vmem_limit_bytes=VMEM_LIMIT),
        name="tensor_gather_%d" % cid,
    )(block)


def scatter_kernel(p_ref, o_ref, from_sib, chip_sum, landed, send, recv):
    dp, me, sib, across, diag = places()
    rows = p_ref.shape[0] // 4
    part = rows // PARTS
    greet([(dp, sib), (dp, across)])

    def at(owner, i):
        return pl.ds(pl.multiple_of(owner * rows + i * part, part), part)

    first, last = [], []
    for i in range(PARTS):
        here = pl.ds(i * part, part)
        first.append(remote(p_ref.at[at(diag, i)], from_sib.at[0, here], send.at[i], recv.at[i], (dp, sib)))
        first[-1].start()
    for i in range(PARTS):
        here = pl.ds(i * part, part)
        j = PARTS + i
        last.append(remote(p_ref.at[at(sib, i)], from_sib.at[1, here], send.at[j], recv.at[j], (dp, sib)))
        last[-1].start()
    crossing = []
    for i in range(PARTS):
        here = pl.ds(i * part, part)
        j = 2 * PARTS + i
        first[i].wait_recv()
        chip_sum[here, :] = (p_ref[at(across, i), :].astype(F32) + from_sib[0, here, :].astype(F32)).astype(BF16)
        crossing.append(remote(chip_sum.at[here], landed.at[here], send.at[j], recv.at[j], (dp, across)))
        crossing[-1].start()
    for i in range(PARTS):
        here = pl.ds(i * part, part)
        last[i].wait_recv()
        o_ref[here, :] = p_ref[at(me, i), :].astype(F32) + from_sib[1, here, :].astype(F32)
    for i in range(PARTS):
        here = pl.ds(i * part, part)
        crossing[i].wait_recv()
        o_ref[here, :] = o_ref[here, :] + landed[here, :].astype(F32)
    for copy in first + last + crossing:
        copy.wait_send()


def tensor_scatter(partial, cid):
    rows, width = partial.shape[0] // 4, partial.shape[1]
    return pl.pallas_call(
        scatter_kernel,
        out_shape=jax.ShapeDtypeStruct((rows, width), F32),
        in_specs=whole_vmem(1),
        out_specs=pl.BlockSpec(memory_space=pltpu.VMEM),
        scratch_shapes=[
            pltpu.VMEM((2, rows, width), BF16),
            pltpu.VMEM((rows, width), BF16),
            pltpu.VMEM((rows, width), BF16),
            pltpu.SemaphoreType.DMA((3 * PARTS,)),
            pltpu.SemaphoreType.DMA((3 * PARTS,)),
        ],
        compiler_params=pltpu.CompilerParams(collective_id=cid, has_side_effects=True, vmem_limit_bytes=VMEM_LIMIT),
        name="tensor_scatter_%d" % cid,
    )(partial)


def dp_lines(count):
    sizes, limit = [], 2
    while count > 1:
        size = min(count, limit)
        sizes.append(size)
        count //= size
        limit *= 2
    return sizes


class Line:
    def __init__(self, size, stride, dp, me):
        self.size = size
        self.place = (dp // stride) % size
        self.right = (jnp.minimum(dp + stride, dp + (size - 1 - self.place) * stride), me)
        self.left = (jnp.maximum(dp - stride, dp - self.place * stride), me)
        self.pair = (dp + stride - 2 * stride * (dp // stride % 2), me)


def lines_of(count, dp, me):
    found, stride = [], 1
    for size in dp_lines(count):
        found.append(Line(size, stride, dp, me))
        stride *= size
    return found


def chunk_sems(count):
    sizes = dp_lines(count)
    return 1 + sizes[1] + sum(4 * size for size in sizes[1:])


def chunk_scratch(count, rows, width):
    sizes = dp_lines(count)
    shapes = [pltpu.VMEM((rows // 2, width), BF16), pltpu.VMEM((rows // 2, width), BF16)]
    part = rows // 2
    for size in sizes[1:]:
        part //= size
        shapes += [pltpu.VMEM((size, part, width), BF16)] * 2
    return shapes


def sum_chunk(lines, x_ref, o_ref, columns, scratch, send, recv):
    rows = x_ref.shape[0]
    got, own = scratch[0], scratch[1]
    buffers = [scratch[2 + 2 * i : 4 + 2 * i] for i in range(len(lines) - 1)]
    pair = lines[0]
    half = rows // 2
    started = []
    used = [0]

    def slots(count):
        used[0] += count
        return used[0] - count

    def go(copy, condition=None):
        if condition is None:
            copy.start()
        else:
            pl.when(condition)(lambda: copy.start())
        started.append((copy, condition))

    def when(condition, body):
        pl.when(condition)(body)

    mine = pl.multiple_of(pair.place * half, half)
    other = pl.multiple_of(half - pair.place * half, half)
    slot = slots(1)
    first = remote(x_ref.at[pl.ds(other, half), columns], got, send.at[slot], recv.at[slot], pair.pair)
    go(first)
    yield
    first.wait_recv()
    own[...] = (x_ref[pl.ds(mine, half), columns].astype(F32) + got[...].astype(F32)).astype(BF16)
    base = 0
    size_now = half
    for line, (to_right, to_left) in zip(lines[1:], buffers):
        n, z = line.size, line.place
        part = size_now // n
        right_slot, left_slot = slots(n), slots(n)
        bases = base

        def piece(o, part=part, bases=bases):
            return pl.ds(pl.multiple_of(bases + o * part, part), part)

        for j in range(n - 1, 0, -1):
            for way in (0, 1):
                o = z + j if way == 0 else z - j
                inside = (o < n) if way == 0 else (o >= 0)
                buffer = to_right if way == 0 else to_left
                at_end = (z == 0) if way == 0 else (z == n - 1)
                slot = (right_slot if way == 0 else left_slot) + jnp.clip(o, 0, n - 1)
                o = jnp.clip(o, 0, n - 1)
                there = line.right if way == 0 else line.left
                copy = remote(own.at[piece(o)], buffer.at[o], send.at[slot], recv.at[slot], there)
                onward = remote(buffer.at[o], buffer.at[o], send.at[slot], recv.at[slot], there)
                go(copy, inside & at_end)

                def pass_on(buffer=buffer, o=o, onward=onward, piece=piece):
                    onward.wait_recv()
                    buffer[o] = (buffer[o].astype(F32) + own[piece(o), :].astype(F32)).astype(BF16)
                    onward.start()

                when(inside & jnp.logical_not(at_end), pass_on)
                started.append((onward, inside & jnp.logical_not(at_end)))
            yield

        def take(buffer, slot, line=line, piece=piece, z=z):
            remote(buffer.at[z], buffer.at[z], send.at[slot + z], recv.at[slot + z], line.right).wait_recv()
            own[piece(z), :] = (own[piece(z), :].astype(F32) + buffer[z].astype(F32)).astype(BF16)

        when(z > 0, functools.partial(take, to_right, right_slot))
        when(z < n - 1, functools.partial(take, to_left, left_slot))
        base = bases + z * part
        size_now = part
    final = pl.ds(pl.multiple_of(mine + base, size_now), size_now)
    o_ref[final, columns] = own[pl.ds(pl.multiple_of(base, size_now), size_now), :]
    region = mine + base
    for level in range(len(lines) - 1, 0, -1):
        line = lines[level]
        n, z = line.size, line.place
        part = size_now
        base_region = region - z * part
        right_slot, left_slot = slots(n), slots(n)
        pair_slot = slots(n) if level == 1 else None

        def piece(o, part=part, base_region=base_region):
            return pl.ds(pl.multiple_of(base_region + o * part, part), part)

        def copy_of(o, slot, there, piece=piece):
            ref = o_ref.at[piece(o), columns]
            return remote(ref, ref, send.at[slot + o], recv.at[slot + o], there)

        go(copy_of(z, right_slot, line.right), z < n - 1)
        go(copy_of(z, left_slot, line.left), z > 0)
        if level == 1:
            go(copy_of(z, pair_slot, pair.pair))
        yield
        for j in range(1, n):
            for way in (0, 1):
                o = z - j if way == 0 else z + j
                inside = (o >= 0) if way == 0 else (o < n)
                goes_on = (z < n - 1) if way == 0 else (z > 0)
                o = jnp.clip(o, 0, n - 1)
                slot = right_slot if way == 0 else left_slot
                there = line.right if way == 0 else line.left
                copy = copy_of(o, slot, there)
                when(inside, lambda copy=copy: copy.wait_recv())
                go(copy, inside & goes_on)
                if level == 1:
                    go(copy_of(o, pair_slot, pair.pair), inside)
            yield
        region = base_region
        size_now = part * n
        if level == 1:
            for o in range(n):
                ref = o_ref.at[pl.ds(pl.multiple_of(other + o * part, part), part), columns]
                remote(ref, ref, send.at[pair_slot + o], recv.at[pair_slot + o], pair.pair).wait_recv()
    for copy, condition in started:
        if condition is None:
            copy.wait_send()
        else:
            when(condition, lambda copy=copy: copy.wait_send())


def run_skewed(makers):
    makers = list(makers)
    running = []
    while makers or running:
        if makers:
            running.append(makers.pop(0)())
        still = []
        for generator in running:
            try:
                next(generator)
                still.append(generator)
            except StopIteration:
                pass
        running = still


def dp_sum_kernel(count, widths, *refs):
    arrays = len(widths)
    ins, rest = refs[:arrays], refs[arrays:]
    vec_ref, bias_ref, pick_ref = rest[:3]
    outs, rest = rest[3 : 3 + arrays], rest[3 + arrays :]
    small_out, rest = rest[0], rest[1:]
    small_in, vec_got, vec_send, vec_recv = rest[:4]
    rest = rest[4:]
    dp, me, sib, across, diag = places()
    lines = lines_of(count, dp, me)
    others = [lines[0].pair]
    near = [(dp, sib), (dp, across), (dp, diag)]
    barrier = pltpu.get_barrier_semaphore()
    for partner in near + others:
        pl.semaphore_signal(barrier, inc=1, device_id=partner, device_id_type=MESH)
    waits = len(near) + len(others)
    for line in lines[1:]:
        has_right = line.place < line.size - 1
        has_left = line.place > 0
        for partner, has in ((line.right, has_right), (line.left, has_left)):
            pl.when(has)(
                lambda partner=partner: pl.semaphore_signal(
                    barrier, inc=1, device_id=partner, device_id_type=MESH
                )
            )
        waits = waits + has_right.astype(jnp.int32) + has_left.astype(jnp.int32)
    pl.semaphore_wait(barrier, waits)
    vec_copies = []
    for i, device in enumerate(near):
        vec_copies.append(remote(vec_ref, vec_got.at[i], vec_send.at[i], vec_recv.at[i], device))
        vec_copies[-1].start()

    per = 2 + 2 * (len(lines) - 1)
    makers = []
    for array in range(arrays):
        wide = ins[array].shape[1]
        for start in range(0, wide, widths[array]):
            scratch, rest = rest[:per], rest[per:]
            send, recv = rest[:2]
            rest = rest[2:]
            makers.append(
                functools.partial(
                    sum_chunk, lines, ins[array], outs[array], pl.ds(start, widths[array]), scratch, send, recv
                )
            )

    def small():
        for copy in vec_copies:
            copy.wait_recv()
        total = vec_ref[...] + vec_got[0] + vec_got[1] + vec_got[2]
        sections = pick_ref.shape[0]
        for s in range(sections):
            small_in[pl.ds(32 * s, 32), :] = (total[0:32] * pick_ref[s : s + 1, :]).astype(BF16)
        small_in[pl.ds(32 * sections, 16), :] = total[32:48].astype(BF16)
        small_in[pl.ds(32 * sections + 16, 16), :] = bias_ref[...].astype(BF16)
        done = 32 * sections + 32
        if done < small_in.shape[0]:
            small_in[pl.ds(done, small_in.shape[0] - done), :] = jnp.zeros((small_in.shape[0] - done, 128), BF16)
        yield from sum_chunk(lines, small_in, small_out, slice(None), rest[:per], rest[per], rest[per + 1])

    run_skewed(makers + [small])
    for copy in vec_copies:
        copy.wait_send()


def dp_sum(count, grads, widths, vec, bias, pick, cid):
    small_rows = max(16 * count, -(-(32 * pick.shape[0] + 32) // (16 * count)) * 16 * count)
    sems = chunk_sems(count)
    scratch = [
        pltpu.VMEM((small_rows, 128), BF16),
        pltpu.VMEM((3,) + vec.shape, F32),
        pltpu.SemaphoreType.DMA((3,)),
        pltpu.SemaphoreType.DMA((3,)),
    ]
    for grad, width in zip(grads, widths):
        for _ in range(0, grad.shape[1], width):
            scratch += chunk_scratch(count, grad.shape[0], width)
            scratch += [pltpu.SemaphoreType.DMA((sems,))] * 2
    scratch += chunk_scratch(count, small_rows, 128)
    scratch += [pltpu.SemaphoreType.DMA((sems,))] * 2
    return pl.pallas_call(
        functools.partial(dp_sum_kernel, count, tuple(widths)),
        out_shape=[jax.ShapeDtypeStruct(g.shape, BF16) for g in grads]
        + [jax.ShapeDtypeStruct((small_rows, 128), BF16)],
        in_specs=whole_vmem(len(grads) + 3),
        out_specs=whole_vmem(len(grads) + 1),
        scratch_shapes=scratch,
        compiler_params=pltpu.CompilerParams(collective_id=cid, has_side_effects=True, vmem_limit_bytes=VMEM_LIMIT),
        name="dp_sum",
    )(*grads, vec, bias, pick)


class Turns:
    def __init__(self, generators):
        self.waiting = list(generators)
        self.running = []
        for generator in self.waiting:
            next(generator)

    def turn(self):
        if self.waiting:
            self.running.append(self.waiting.pop(0))
        still = []
        for generator in self.running:
            try:
                next(generator)
                still.append(generator)
            except StopIteration:
                pass
        self.running = still

    def drain(self):
        while self.waiting or self.running:
            self.turn()


class Scatter:
    def __init__(self, spot, p_ref, from_sib, chip_sum, landed, send, recv):
        self.dp, self.me, self.sib, self.across, self.diag = spot
        self.rows = p_ref.shape[0] // 4
        self.part = self.rows // PARTS
        self.p_ref, self.from_sib, self.chip_sum, self.landed = p_ref, from_sib, chip_sum, landed

        def near(owner, which, i):
            slot = which * PARTS + i
            return remote(
                p_ref.at[self.at(owner, i)],
                from_sib.at[which, self.here(i)],
                send.at[slot],
                recv.at[slot],
                (self.dp, self.sib),
            )

        self.first = [near(self.diag, 0, i) for i in range(PARTS)]
        self.last = [near(self.sib, 1, i) for i in range(PARTS)]
        self.crossing = [
            remote(
                chip_sum.at[self.here(i)],
                landed.at[self.here(i)],
                send.at[2 * PARTS + i],
                recv.at[2 * PARTS + i],
                (self.dp, self.across),
            )
            for i in range(PARTS)
        ]

    def here(self, i):
        return pl.ds(i * self.part, self.part)

    def at(self, owner, i):
        return pl.ds(pl.multiple_of(owner * self.rows + i * self.part, self.part), self.part)

    def start_first(self):
        for copy in self.first:
            copy.start()

    def start_last(self):
        for copy in self.last:
            copy.start()

    def cross(self):
        for i in range(PARTS):
            self.first[i].wait_recv()
            self.chip_sum[self.here(i), :] = (
                self.p_ref[self.at(self.across, i), :].astype(F32) + self.from_sib[0, self.here(i), :].astype(F32)
            ).astype(BF16)
            self.crossing[i].start()

    def result(self, i):
        self.last[i].wait_recv()
        total = self.p_ref[self.at(self.me, i), :].astype(F32) + self.from_sib[1, self.here(i), :].astype(F32)
        self.crossing[i].wait_recv()
        return total + self.landed[self.here(i), :].astype(F32)

    def finish(self):
        for copy in self.first + self.last + self.crossing:
            copy.wait_send()


def late_kernel(count, width, *refs):
    p_ref, normed_ref, inverse_ref, cot_ref, gain_ref, w_out_ref = refs[:6]
    q_ref, k_ref, kt_ref, v_ref, log_ref, bias_ref = refs[6:12]
    wq_ref, wk_ref, wv_ref, gi_ref, go_ref = refs[12:17]
    gsec_ref, ghid_ref, gattn_ref, dq_ref, dk_ref, dv_ref, gfirst_ref, si_ref, so_ref = refs[17:26]
    rest = refs[26:]
    from_one, chip_one, landed_one, send_one, recv_one = rest[:5]
    from_two, chip_two, landed_two, send_two, recv_two = rest[5:10]
    total_ref, gsend, grecv = rest[10:13]
    do_cat, q_cat, p_scr, ds_scr, dk_acc, dv_acc, dqt_ref = rest[13:20]
    rest = rest[20:]
    spot = places()
    dp, me, sib, across, diag = spot
    lines = lines_of(count, dp, me)
    barrier = pltpu.get_barrier_semaphore()
    for partner in [(dp, sib), (dp, across), lines[0].pair]:
        pl.semaphore_signal(barrier, inc=1, device_id=partner, device_id_type=MESH)
    waits = 3
    for line in lines[1:]:
        has_right = line.place < line.size - 1
        has_left = line.place > 0
        for partner, has in ((line.right, has_right), (line.left, has_left)):
            pl.when(has)(
                lambda partner=partner: pl.semaphore_signal(
                    barrier, inc=1, device_id=partner, device_id_type=MESH
                )
            )
        waits = waits + has_right.astype(jnp.int32) + has_left.astype(jnp.int32)
    pl.semaphore_wait(barrier, waits)

    rows = normed_ref.shape[0]
    one = Scatter(spot, p_ref, from_one, chip_one, landed_one, send_one, recv_one)
    one.start_first()
    one.start_last()
    per = 2 + 2 * (len(lines) - 1)
    chunks = []
    for x_ref, o_ref in ((gi_ref, si_ref), (go_ref, so_ref)):
        for start in range(0, x_ref.shape[1], width):
            chunks.append(
                sum_chunk(lines, x_ref, o_ref, pl.ds(start, width), rest[:per], rest[per], rest[per + 1])
            )
            rest = rest[per + 2 :]
    turns = Turns(chunks)
    one.cross()

    dk_acc[...] = jnp.zeros_like(dk_acc)
    dv_acc[...] = jnp.zeros_like(dv_acc)
    part = rows // PARTS
    to_across, to_sib, passed = [], [], []

    def block_part(owner, i):
        return gattn_ref.at[pl.ds(pl.multiple_of(owner * rows + i * part, part), part)]

    for i in range(PARTS):
        here = pl.ds(i * part, part)
        grad_second = one.result(i)
        gsec_ref[here, :] = grad_second
        normed = normed_ref[here, :]
        grad_hat = grad_second * gain_ref[...]
        back = inverse_ref[here, :] * (
            grad_hat
            - jnp.mean(grad_hat, axis=-1, keepdims=True)
            - normed * jnp.mean(grad_hat * normed, axis=-1, keepdims=True)
        )
        grad_hidden = cot_ref[here, :].astype(F32) + back
        ghid_ref[here, :] = grad_hidden
        gattn_ref[pl.ds(pl.multiple_of(me * rows + i * part, part), part), :] = grad_hidden.astype(BF16)
        ref = block_part(me, i)
        to_across.append(remote(ref, ref, gsend.at[i], grecv.at[i], (dp, across)))
        to_across[-1].start()
        to_sib.append(remote(ref, ref, gsend.at[PARTS + i], grecv.at[PARTS + i], (dp, sib)))
        to_sib[-1].start()
    turns.turn()

    heads = q_ref.shape[1] // HDIM
    scale = HDIM ** (-0.5)
    lanes = lax.broadcasted_iota(jnp.int32, (rows, q_ref.shape[1]), 1) // HDIM

    def attend(owner):
        block = pl.ds(pl.multiple_of(owner * rows, rows), rows)
        grad_att = dot(gattn_ref[block, :], w_out_ref[...], ((1,), (1,))).astype(BF16)
        query = q_ref[block, :]
        for h in range(heads):
            do_cat[pl.ds(h * rows, rows), :] = jnp.where(lanes == h, grad_att, jnp.zeros_like(grad_att))
            q_cat[pl.ds(h * rows, rows), :] = jnp.where(lanes == h, query, jnp.zeros_like(query))

        @pl.loop(0, heads)
        def _(h):
            at = pl.ds(pl.multiple_of(h * rows, rows), rows)
            scores = dot(k_ref[...], q_cat[at, :], ((1,), (1,)))
            probs = jnp.exp(scores * scale + (bias_ref[...] - log_ref[owner * heads + h]))
            grad_probs = dot(v_ref[...], do_cat[at, :], ((1,), (1,)))
            centre = jnp.sum(probs * grad_probs, axis=0, keepdims=True)
            grad_scores = (probs * (grad_probs - centre)).astype(BF16)
            p_scr[:, at] = probs.astype(BF16)
            ds_scr[:, at] = grad_scores
            head = pl.ds(pl.multiple_of(h * HDIM, HDIM), HDIM)
            dqt_ref[owner, head, :] = dot(kt_ref[head, :], grad_scores, ((1,), (0,)))

        dv_acc[...] += dot(p_scr[...], do_cat[...], ((1,), (0,)))
        dk_acc[...] += dot(ds_scr[...], q_cat[...], ((1,), (0,)))

    def pass_on(i):
        to_across[i].wait_recv()
        ref = block_part(across, i)
        passed.append(remote(ref, ref, gsend.at[2 * PARTS + i], grecv.at[2 * PARTS + i], (dp, sib)))
        passed[-1].start()

    attend(me)
    turns.turn()
    pass_on(0)
    pass_on(1)
    for copy in to_sib:
        copy.wait_recv()
    attend(sib)
    pass_on(2)
    pass_on(3)
    turns.turn()
    attend(across)
    turns.turn()
    for copy in passed:
        copy.wait_recv()
    attend(diag)
    turns.turn()

    dk_ref[...] = (dk_acc[...] * scale).astype(BF16)
    dv_ref[...] = dv_acc[...].astype(BF16)
    two = Scatter(spot, total_ref, from_two, chip_two, landed_two, send_two, recv_two)

    def total(owner):
        block = pl.ds(pl.multiple_of(owner * rows, rows), rows)
        grad_query = (dqt_ref[owner].T * scale).astype(BF16)
        dq_ref[block, :] = grad_query
        total_ref[block, :] = (
            dot(grad_query, wq_ref[...], ((1,), (1,)))
            + dot(dk_ref[block, :], wk_ref[...], ((1,), (1,)))
            + dot(dv_ref[block, :], wv_ref[...], ((1,), (1,)))
        ).astype(BF16)

    total(diag)
    two.start_first()
    total(across)
    two.cross()
    total(sib)
    two.start_last()
    total(me)
    turns.turn()
    for i in range(PARTS):
        gfirst_ref[pl.ds(i * part, part), :] = two.result(i)
    turns.drain()
    one.finish()
    two.finish()
    for copy in to_across + to_sib + passed:
        copy.wait_send()


def late(count, width, cid, *operands):
    normed, q, gi, go = operands[1], operands[6], operands[15], operands[16]
    rows, model = normed.shape
    seq, local = q.shape
    heads = local // HDIM
    sems = chunk_sems(count)

    def dma(n):
        return [pltpu.SemaphoreType.DMA((n,))] * 2

    def scatter_scratch():
        return [
            pltpu.VMEM((2, rows, model), BF16),
            pltpu.VMEM((rows, model), BF16),
            pltpu.VMEM((rows, model), BF16),
        ] + dma(3 * PARTS)

    scratch = scatter_scratch() + scatter_scratch()
    scratch += [pltpu.VMEM((seq, model), BF16)] + dma(3 * PARTS)
    scratch += [
        pltpu.VMEM((heads * rows, local), BF16),
        pltpu.VMEM((heads * rows, local), BF16),
        pltpu.VMEM((seq, heads * rows), BF16),
        pltpu.VMEM((seq, heads * rows), BF16),
        pltpu.VMEM((seq, local), F32),
        pltpu.VMEM((seq, local), F32),
        pltpu.VMEM((seq // rows, local, rows), F32),
    ]
    for grad in (gi, go):
        for _ in range(0, grad.shape[1], width):
            scratch += chunk_scratch(count, grad.shape[0], width) + dma(sems)
    shape = jax.ShapeDtypeStruct
    return pl.pallas_call(
        functools.partial(late_kernel, count, width),
        out_shape=[
            shape((rows, model), F32),
            shape((rows, model), F32),
            shape((seq, model), BF16),
            shape((seq, local), BF16),
            shape((seq, local), BF16),
            shape((seq, local), BF16),
            shape((rows, model), F32),
            shape(gi.shape, BF16),
            shape(go.shape, BF16),
        ],
        in_specs=whole_vmem(len(operands)),
        out_specs=whole_vmem(9),
        scratch_shapes=scratch,
        compiler_params=pltpu.CompilerParams(collective_id=cid, has_side_effects=True, vmem_limit_bytes=VMEM_LIMIT),
        name="late",
    )(*operands)


def normalize(row_block):
    centered = row_block - jnp.mean(row_block, axis=-1, keepdims=True)
    inverse = lax.rsqrt(jnp.mean(centered * centered, axis=-1, keepdims=True) + EPSILON)
    return (centered * inverse, inverse)


def norm_back(grad_hat, normed, inverse):
    return inverse * (
        grad_hat
        - jnp.mean(grad_hat, axis=-1, keepdims=True)
        - normed * jnp.mean(grad_hat * normed, axis=-1, keepdims=True)
    )


def exact_gelu(values):
    return jax.nn.gelu(values, approximate=False)


def split_heads(flat_rows):
    return flat_rows.reshape(-1, SEQ, flat_rows.shape[1] // HDIM, HDIM)


def dot(a, b, dims):
    return lax.dot_general(a, b, (dims, ((), ())), preferred_element_type=F32)


def masked_scores(query_block, keys_all, valid_keys, score_scale):
    scores = jnp.einsum("sqhe,skhe->shqk", query_block, keys_all, preferred_element_type=F32) * score_scale
    return jnp.where(valid_keys[:, None, None, :], scores, NEG_LARGE)


def attention_forward(queries, keys_all, values_all, valid_keys, score_scale, block_rows):
    pieces = []
    log_sums = []
    for offset in range(0, SEQ, block_rows):
        scores = masked_scores(queries[:, offset : offset + block_rows], keys_all, valid_keys, score_scale)
        highest = jnp.max(scores, axis=-1, keepdims=True)
        weights = jnp.exp(scores - highest)
        totals = jnp.sum(weights, axis=-1, keepdims=True)
        softmax_low = (weights / totals).astype(BF16)
        mixture = jnp.einsum("shqk,skhe->sqhe", softmax_low, values_all, preferred_element_type=F32)
        pieces.append(mixture.astype(BF16))
        log_sums.append((highest + jnp.log(totals))[..., 0])
    return (jnp.concatenate(pieces, axis=1), jnp.concatenate(log_sums, axis=2))


def body(
    dp_count,
    frames,
    cotangent,
    ada_gain,
    ada_shift,
    w_query,
    b_query,
    w_key,
    w_value,
    b_value,
    w_out,
    b_out,
    w_inner,
    b_inner,
    w_outer,
    b_outer,
    section_index,
    lengths,
    key_mask,
):
    rows_dev, width = frames.shape
    sections = ada_gain.shape[0]
    assert section_index.shape[0] == 1
    score_scale = HDIM ** (-0.5)
    block_rows = 512
    section = section_index[0] - 2
    gain = lax.dynamic_slice(ada_gain, (section, 0), (1, 2 * width))
    shift = lax.dynamic_slice(ada_shift, (section, 0), (1, 2 * width))
    pick = jnp.broadcast_to(
        (section == jnp.arange(sections, dtype=jnp.int32)).astype(F32)[:, None], (sections, 128)
    )
    spots = jnp.arange(SEQ, dtype=jnp.int32)
    valid_keys = (spots[None, :] < lengths[:, None]) & (key_mask.reshape(1, SEQ) > 0)
    inputs = frames.astype(F32)
    normed_one, inverse_one = normalize(inputs)
    first_low = (normed_one * gain[:, :width] + shift[:, :width]).astype(BF16)
    first_all = tensor_gather(first_low, 1)
    queries = (dot(first_all, w_query, ((1,), (0,))) + b_query).astype(BF16)
    keys_all = dot(first_all, w_key, ((1,), (0,))).astype(BF16)
    values_all = (dot(first_all, w_value, ((1,), (0,))) + b_value).astype(BF16)
    attended_heads, log_sums = attention_forward(
        split_heads(queries), split_heads(keys_all), split_heads(values_all), valid_keys, score_scale, block_rows
    )
    attended = attended_heads.reshape(queries.shape)
    hidden = inputs + tensor_scatter(dot(attended, w_out, ((1,), (0,))).astype(BF16), 2) + b_out
    normed_two, inverse_two = normalize(hidden)
    second_low = (normed_two * gain[:, width:] + shift[:, width:]).astype(BF16)
    second_all = tensor_gather(second_low, 3)
    grad_all = tensor_gather(cotangent, 4)
    inner_pre = dot(second_all, w_inner, ((1,), (0,))) + b_inner
    activated = exact_gelu(inner_pre).astype(BF16)
    layer_out = (
        hidden + tensor_scatter(dot(activated, w_outer, ((1,), (0,))).astype(BF16), 5) + b_outer
    ).astype(BF16)
    grad_w_outer = dot(activated, grad_all, ((0,), (0,))).astype(BF16)
    grad_activated = dot(grad_all, w_outer, ((1,), (1,)))
    unused_value, gelu_pull = jax.vjp(exact_gelu, inner_pre)
    grad_inner = gelu_pull(grad_activated)[0].astype(BF16)
    grad_w_inner = dot(second_all, grad_inner, ((0,), (0,))).astype(BF16)
    grad_b_inner = jnp.sum(grad_inner.astype(F32), axis=0)
    second_part = dot(grad_inner, w_inner, ((1,), (1,))).astype(BF16)
    bias_keys = jnp.broadcast_to(jnp.where(valid_keys[0], 0.0, NEG_LARGE)[:, None], (SEQ, rows_dev))
    heads_here = w_query.shape[1] // HDIM
    logs = log_sums.reshape(heads_here, SEQ // rows_dev, rows_dev).transpose(1, 0, 2)
    (
        grad_second,
        grad_hidden,
        grad_attn_all,
        grad_queries,
        grad_keys,
        grad_values,
        grad_first,
        sum_inner,
        sum_outer,
    ) = late(
        dp_count,
        512,
        6,
        second_part,
        normed_two,
        inverse_two,
        cotangent,
        gain[:, width:],
        w_out,
        queries,
        keys_all,
        keys_all.T,
        values_all,
        logs.reshape(-1, 1, rows_dev),
        bias_keys,
        w_query,
        w_key,
        w_value,
        grad_w_inner,
        grad_w_outer,
    )
    grad_out_rows = cotangent.astype(F32)
    grad_w_out = dot(grad_attn_all, attended, ((0,), (0,)))
    grad_b_query = jnp.sum(grad_queries.astype(F32), axis=0)
    grad_b_value = jnp.sum(grad_values.astype(F32), axis=0)
    grad_w_attn = jnp.concatenate(
        [
            dot(first_all, grad_queries, ((0,), (0,))).astype(BF16),
            dot(first_all, grad_keys, ((0,), (0,))).astype(BF16),
            dot(first_all, grad_values, ((0,), (0,))).astype(BF16),
            grad_w_out.astype(BF16),
        ],
        axis=1,
    )
    frames_grad = grad_hidden + norm_back(grad_first * gain[:, :width], normed_one, inverse_one)
    vec = jnp.concatenate(
        [
            jnp.sum(grad_first * normed_one, axis=0),
            jnp.sum(grad_second * normed_two, axis=0),
            jnp.sum(grad_first, axis=0),
            jnp.sum(grad_second, axis=0),
            jnp.sum(grad_hidden, axis=0),
            jnp.sum(grad_out_rows, axis=0),
        ]
    ).reshape(-1, 128)
    bias = jnp.concatenate(
        [grad_b_inner, grad_b_query, grad_b_value, jnp.zeros((2048 - 1024 - 512,), F32)]
    ).reshape(16, 128)
    sum_attn, small = dp_sum(dp_count, [grad_w_attn], [256], vec, bias, pick, 9)
    small = small.astype(F32)
    tables = small[: 32 * sections].reshape(sections, 2, 2 * width)
    shared = small[32 * sections : 32 * sections + 16].reshape(2, width)
    biases = small[32 * sections + 16 : 32 * sections + 32].reshape(-1)
    heads = w_query.shape[1]
    units = w_inner.shape[1]
    return (
        layer_out,
        frames_grad,
        tables[:, 0],
        tables[:, 1],
        sum_attn[:, :heads].astype(F32),
        biases[units : units + heads],
        sum_attn[:, heads : 2 * heads].astype(F32),
        sum_attn[:, 2 * heads : 3 * heads].astype(F32),
        biases[units + heads : units + 2 * heads],
        sum_attn[:, 3 * heads :].T.astype(F32),
        shared[0],
        sum_inner.astype(F32),
        biases[:units],
        sum_outer.astype(F32),
        shared[1],
    )


def solution(mesh):
    return jax.shard_map(
        functools.partial(body, mesh.shape["dp"]),
        mesh=mesh,
        in_specs=(
            P(("dp", "tensor"), None),
            P(("dp", "tensor"), None),
            P(),
            P(),
            P(None, "tensor"),
            P("tensor"),
            P(None, "tensor"),
            P(None, "tensor"),
            P("tensor"),
            P("tensor", None),
            P(),
            P(None, "tensor"),
            P("tensor"),
            P("tensor", None),
            P(),
            P("dp"),
            P("dp"),
            P("dp"),
        ),
        out_specs=(
            P(("dp", "tensor"), None),
            P(("dp", "tensor"), None),
            P(),
            P(),
            P(None, "tensor"),
            P("tensor"),
            P(None, "tensor"),
            P(None, "tensor"),
            P("tensor"),
            P("tensor", None),
            P(),
            P(None, "tensor"),
            P("tensor"),
            P("tensor", None),
            P(),
        ),
        check_vma=False,
    )
```

```python
import functools

import jax
import jax.numpy as jnp
from jax import lax
from jax.experimental import pallas as pl
from jax.experimental.pallas import tpu as pltpu
from jax.sharding import PartitionSpec as P

HDIM = 64
SEQ = 1024
EPSILON = 1e-05
NEG_LARGE = -1e30
F32 = jnp.float32
BF16 = jnp.bfloat16
MESH = pl.DeviceIdType.MESH
VMEM_LIMIT = 60 * 1024 * 1024


def places():
    dp = lax.axis_index("dp")
    me = lax.axis_index("tensor")
    sib = me + 1 - 2 * (me % 2)
    across = (me + 2) % 4
    diag = (sib + 2) % 4
    return dp, me, sib, across, diag


def greet(partners):
    barrier = pltpu.get_barrier_semaphore()
    for partner in partners:
        pl.semaphore_signal(barrier, inc=1, device_id=partner, device_id_type=MESH)
    pl.semaphore_wait(barrier, len(partners))


def remote(src, dst, send, recv, device):
    return pltpu.make_async_remote_copy(
        src_ref=src, dst_ref=dst, send_sem=send, recv_sem=recv, device_id=device, device_id_type=MESH
    )


def whole_vmem(count):
    return [pl.BlockSpec(memory_space=pltpu.VMEM)] * count


PARTS = 4


def gather_kernel(x_ref, o_ref, send, recv):
    dp, me, sib, across, diag = places()
    rows = x_ref.shape[0]
    part = rows // PARTS
    greet([(dp, sib), (dp, across)])
    copies = []
    for i in range(PARTS):
        at = pl.multiple_of(me * rows + i * part, part)
        copies.append(
            remote(x_ref.at[pl.ds(i * part, part)], o_ref.at[pl.ds(at, part)], send.at[i], recv.at[i], (dp, across))
        )
        copies[-1].start()
    mine = pl.ds(pl.multiple_of(me * rows, rows), rows)
    copies.append(remote(x_ref, o_ref.at[mine], send.at[PARTS], recv.at[PARTS], (dp, sib)))
    copies[-1].start()
    o_ref[mine, :] = x_ref[...]
    for i in range(PARTS):
        copies[i].wait_recv()
        there = pl.ds(pl.multiple_of(across * rows + i * part, part), part)
        j = PARTS + 1 + i
        copies.append(remote(o_ref.at[there], o_ref.at[there], send.at[j], recv.at[j], (dp, sib)))
        copies[-1].start()
    for i, copy in enumerate(copies):
        if i >= PARTS:
            copy.wait_recv()
        copy.wait_send()


def tensor_gather(block, cid):
    rows, width = block.shape
    return pl.pallas_call(
        gather_kernel,
        out_shape=jax.ShapeDtypeStruct((rows * 4, width), block.dtype),
        in_specs=whole_vmem(1),
        out_specs=pl.BlockSpec(memory_space=pltpu.VMEM),
        scratch_shapes=[pltpu.SemaphoreType.DMA((2 * PARTS + 1,))] * 2,
        compiler_params=pltpu.CompilerParams(collective_id=cid, has_side_effects=True, vmem_limit_bytes=VMEM_LIMIT),
        name="tensor_gather_%d" % cid,
    )(block)


def scatter_kernel(p_ref, o_ref, from_sib, chip_sum, landed, send, recv):
    dp, me, sib, across, diag = places()
    rows = p_ref.shape[0] // 4
    part = rows // PARTS
    greet([(dp, sib), (dp, across)])

    def at(owner, i):
        return pl.ds(pl.multiple_of(owner * rows + i * part, part), part)

    first, last = [], []
    for i in range(PARTS):
        here = pl.ds(i * part, part)
        first.append(remote(p_ref.at[at(diag, i)], from_sib.at[0, here], send.at[i], recv.at[i], (dp, sib)))
        first[-1].start()
    for i in range(PARTS):
        here = pl.ds(i * part, part)
        j = PARTS + i
        last.append(remote(p_ref.at[at(sib, i)], from_sib.at[1, here], send.at[j], recv.at[j], (dp, sib)))
        last[-1].start()
    crossing = []
    for i in range(PARTS):
        here = pl.ds(i * part, part)
        j = 2 * PARTS + i
        first[i].wait_recv()
        chip_sum[here, :] = (p_ref[at(across, i), :].astype(F32) + from_sib[0, here, :].astype(F32)).astype(BF16)
        crossing.append(remote(chip_sum.at[here], landed.at[here], send.at[j], recv.at[j], (dp, across)))
        crossing[-1].start()
    for i in range(PARTS):
        here = pl.ds(i * part, part)
        last[i].wait_recv()
        o_ref[here, :] = p_ref[at(me, i), :].astype(F32) + from_sib[1, here, :].astype(F32)
    for i in range(PARTS):
        here = pl.ds(i * part, part)
        crossing[i].wait_recv()
        o_ref[here, :] = o_ref[here, :] + landed[here, :].astype(F32)
    for copy in first + last + crossing:
        copy.wait_send()


def tensor_scatter(partial, cid):
    rows, width = partial.shape[0] // 4, partial.shape[1]
    return pl.pallas_call(
        scatter_kernel,
        out_shape=jax.ShapeDtypeStruct((rows, width), F32),
        in_specs=whole_vmem(1),
        out_specs=pl.BlockSpec(memory_space=pltpu.VMEM),
        scratch_shapes=[
            pltpu.VMEM((2, rows, width), BF16),
            pltpu.VMEM((rows, width), BF16),
            pltpu.VMEM((rows, width), BF16),
            pltpu.SemaphoreType.DMA((3 * PARTS,)),
            pltpu.SemaphoreType.DMA((3 * PARTS,)),
        ],
        compiler_params=pltpu.CompilerParams(collective_id=cid, has_side_effects=True, vmem_limit_bytes=VMEM_LIMIT),
        name="tensor_scatter_%d" % cid,
    )(partial)


def dp_lines(count):
    sizes, limit = [], 2
    while count > 1:
        size = min(count, limit)
        sizes.append(size)
        count //= size
        limit *= 2
    return sizes


class Line:
    def __init__(self, size, stride, dp, me):
        self.size = size
        self.place = (dp // stride) % size
        self.right = (jnp.minimum(dp + stride, dp + (size - 1 - self.place) * stride), me)
        self.left = (jnp.maximum(dp - stride, dp - self.place * stride), me)
        self.pair = (dp + stride - 2 * stride * (dp // stride % 2), me)


def lines_of(count, dp, me):
    found, stride = [], 1
    for size in dp_lines(count):
        found.append(Line(size, stride, dp, me))
        stride *= size
    return found


def chunk_sems(count):
    sizes = dp_lines(count)
    return 1 + sizes[1] + sum(4 * size for size in sizes[1:])


def chunk_scratch(count, rows, width):
    sizes = dp_lines(count)
    shapes = [pltpu.VMEM((rows // 2, width), BF16), pltpu.VMEM((rows // 2, width), BF16)]
    part = rows // 2
    for size in sizes[1:]:
        part //= size
        shapes += [pltpu.VMEM((size - 1, part, width), BF16)] * 2
    return shapes


def sum_chunk(lines, x_ref, o_ref, columns, scratch, send, recv):
    rows = x_ref.shape[0]
    got, own = scratch[0], scratch[1]
    buffers = [scratch[2 + 2 * i : 4 + 2 * i] for i in range(len(lines) - 1)]
    pair = lines[0]
    half = rows // 2
    started = []
    used = [0]

    def slots(count):
        used[0] += count
        return used[0] - count

    def go(copy, condition=None):
        if condition is None:
            copy.start()
        else:
            pl.when(condition)(lambda: copy.start())
        started.append((copy, condition))

    def when(condition, body):
        pl.when(condition)(body)

    mine = pl.multiple_of(pair.place * half, half)
    other = pl.multiple_of(half - pair.place * half, half)
    slot = slots(1)
    first = remote(x_ref.at[pl.ds(other, half), columns], got, send.at[slot], recv.at[slot], pair.pair)
    go(first)
    yield
    first.wait_recv()
    own[...] = (x_ref[pl.ds(mine, half), columns].astype(F32) + got[...].astype(F32)).astype(BF16)
    base = 0
    size_now = half
    for line, (to_right, to_left) in zip(lines[1:], buffers):
        n, z = line.size, line.place
        part = size_now // n
        right_slot, left_slot = slots(n), slots(n)
        bases = base

        def piece(o, part=part, bases=bases):
            return pl.ds(pl.multiple_of(bases + o * part, part), part)

        for j in range(n - 1, 0, -1):
            for way in (0, 1):
                o = z + j if way == 0 else z - j
                inside = (o < n) if way == 0 else (o >= 0)
                buffer = to_right if way == 0 else to_left
                at_end = (z == 0) if way == 0 else (z == n - 1)
                slot = (right_slot if way == 0 else left_slot) + jnp.clip(o, 0, n - 1)
                o = jnp.clip(o, 0, n - 1)
                at = jnp.clip(o - 1 + way, 0, n - 2)
                there = line.right if way == 0 else line.left
                copy = remote(own.at[piece(o)], buffer.at[at], send.at[slot], recv.at[slot], there)
                onward = remote(buffer.at[at], buffer.at[at], send.at[slot], recv.at[slot], there)
                go(copy, inside & at_end)

                def pass_on(buffer=buffer, o=o, at=at, onward=onward, piece=piece):
                    onward.wait_recv()
                    buffer[at] = (buffer[at].astype(F32) + own[piece(o), :].astype(F32)).astype(BF16)
                    onward.start()

                when(inside & jnp.logical_not(at_end), pass_on)
                started.append((onward, inside & jnp.logical_not(at_end)))
            yield

        def take(buffer, slot, at, line=line, piece=piece, z=z):
            remote(buffer.at[at], buffer.at[at], send.at[slot + z], recv.at[slot + z], line.right).wait_recv()
            own[piece(z), :] = (own[piece(z), :].astype(F32) + buffer[at].astype(F32)).astype(BF16)

        when(z > 0, functools.partial(take, to_right, right_slot, jnp.maximum(z - 1, 0)))
        when(z < n - 1, functools.partial(take, to_left, left_slot, jnp.minimum(z, n - 2)))
        base = bases + z * part
        size_now = part
    final = pl.ds(pl.multiple_of(mine + base, size_now), size_now)
    o_ref[final, columns] = own[pl.ds(pl.multiple_of(base, size_now), size_now), :]
    region = mine + base
    for level in range(len(lines) - 1, 0, -1):
        line = lines[level]
        n, z = line.size, line.place
        part = size_now
        base_region = region - z * part
        right_slot, left_slot = slots(n), slots(n)
        pair_slot = slots(n) if level == 1 else None

        def piece(o, part=part, base_region=base_region):
            return pl.ds(pl.multiple_of(base_region + o * part, part), part)

        def copy_of(o, slot, there, piece=piece):
            ref = o_ref.at[piece(o), columns]
            return remote(ref, ref, send.at[slot + o], recv.at[slot + o], there)

        go(copy_of(z, right_slot, line.right), z < n - 1)
        go(copy_of(z, left_slot, line.left), z > 0)
        if level == 1:
            go(copy_of(z, pair_slot, pair.pair))
        yield
        for j in range(1, n):
            for way in (0, 1):
                o = z - j if way == 0 else z + j
                inside = (o >= 0) if way == 0 else (o < n)
                goes_on = (z < n - 1) if way == 0 else (z > 0)
                o = jnp.clip(o, 0, n - 1)
                slot = right_slot if way == 0 else left_slot
                there = line.right if way == 0 else line.left
                copy = copy_of(o, slot, there)
                when(inside, lambda copy=copy: copy.wait_recv())
                go(copy, inside & goes_on)
                if level == 1:
                    go(copy_of(o, pair_slot, pair.pair), inside)
            yield
        region = base_region
        size_now = part * n
        if level == 1:
            for o in range(n):
                ref = o_ref.at[pl.ds(pl.multiple_of(other + o * part, part), part), columns]
                remote(ref, ref, send.at[pair_slot + o], recv.at[pair_slot + o], pair.pair).wait_recv()
    for copy, condition in started:
        if condition is None:
            copy.wait_send()
        else:
            when(condition, lambda copy=copy: copy.wait_send())


class Turns:
    def __init__(self, generators):
        self.waiting = list(generators)
        self.running = []
        for generator in self.waiting:
            next(generator)

    def add(self, generator):
        next(generator)
        self.waiting.append(generator)

    def turn(self):
        if self.waiting:
            self.running.append(self.waiting.pop(0))
        still = []
        for generator in self.running:
            try:
                next(generator)
                still.append(generator)
            except StopIteration:
                pass
        self.running = still

    def drain(self):
        while self.waiting or self.running:
            self.turn()


class Scatter:
    def __init__(self, spot, p_ref, from_sib, chip_sum, landed, send, recv):
        self.dp, self.me, self.sib, self.across, self.diag = spot
        self.rows = p_ref.shape[0] // 4
        self.part = self.rows // PARTS
        self.p_ref, self.from_sib, self.chip_sum, self.landed = p_ref, from_sib, chip_sum, landed

        def near(owner, which, i):
            slot = which * PARTS + i
            return remote(
                p_ref.at[self.at(owner, i)],
                from_sib.at[which, self.here(i)],
                send.at[slot],
                recv.at[slot],
                (self.dp, self.sib),
            )

        self.first = [near(self.diag, 0, i) for i in range(PARTS)]
        self.last = [near(self.sib, 1, i) for i in range(PARTS)]
        self.crossing = [
            remote(
                chip_sum.at[self.here(i)],
                landed.at[self.here(i)],
                send.at[2 * PARTS + i],
                recv.at[2 * PARTS + i],
                (self.dp, self.across),
            )
            for i in range(PARTS)
        ]

    def here(self, i):
        return pl.ds(i * self.part, self.part)

    def at(self, owner, i):
        return pl.ds(pl.multiple_of(owner * self.rows + i * self.part, self.part), self.part)

    def start_first(self):
        for copy in self.first:
            copy.start()

    def start_last(self):
        for copy in self.last:
            copy.start()

    def cross(self):
        for i in range(PARTS):
            self.first[i].wait_recv()
            self.chip_sum[self.here(i), :] = (
                self.p_ref[self.at(self.across, i), :].astype(F32) + self.from_sib[0, self.here(i), :].astype(F32)
            ).astype(BF16)
            self.crossing[i].start()

    def result(self, i):
        self.last[i].wait_recv()
        total = self.p_ref[self.at(self.me, i), :].astype(F32) + self.from_sib[1, self.here(i), :].astype(F32)
        self.crossing[i].wait_recv()
        return total + self.landed[self.here(i), :].astype(F32)

    def finish(self):
        for copy in self.first + self.last + self.crossing:
            copy.wait_send()


def norm_parts(block):
    centered = block - jnp.mean(block, axis=-1, keepdims=True)
    inverse = lax.rsqrt(jnp.mean(centered * centered, axis=-1, keepdims=True) + EPSILON)
    return centered * inverse, inverse


def column_sums(block):
    return jnp.sum(block, axis=0, keepdims=True)


def late_kernel(count, width, *refs):
    p_ref, po_ref, hidden_ref, frames_ref, cot_ref, gain_ref, b_outer_ref = refs[:7]
    w_out_ref, q_ref, k_ref, kt_ref, v_ref, log_ref, bias_ref = refs[7:14]
    wq_ref, wk_ref, wv_ref, first_ref, att_ref, gi_ref, go_ref, gb_ref, pick_ref = refs[14:23]
    out_ref, fgrad_ref, si_ref, so_ref, sa_ref, small_ref = refs[23:29]
    rest = refs[29:]
    from_one, chip_one, landed_one, send_one, recv_one = rest[:5]
    from_two, chip_two, landed_two, send_two, recv_two = rest[5:10]
    from_out, chip_out, landed_out, send_out, recv_out = rest[10:15]
    gsend, grecv, vec_got, vec_send, vec_recv = rest[15:20]
    gattn_ref, gsec_ref, ghid_ref, dqkv_ref, vec_ref, small_in = rest[20:26]
    do_cat, q_cat, p_scr, ds_scr, dk_acc, dv_acc, dqt_ref = rest[26:33]
    rest = rest[33:]
    spot = places()
    dp, me, sib, across, diag = spot
    lines = lines_of(count, dp, me)
    barrier = pltpu.get_barrier_semaphore()
    for partner in [(dp, sib), (dp, across), (dp, diag), lines[0].pair]:
        pl.semaphore_signal(barrier, inc=1, device_id=partner, device_id_type=MESH)
    waits = 4
    for line in lines[1:]:
        has_right = line.place < line.size - 1
        has_left = line.place > 0
        for partner, has in ((line.right, has_right), (line.left, has_left)):
            pl.when(has)(
                lambda partner=partner: pl.semaphore_signal(
                    barrier, inc=1, device_id=partner, device_id_type=MESH
                )
            )
        waits = waits + has_right.astype(jnp.int32) + has_left.astype(jnp.int32)
    pl.semaphore_wait(barrier, waits)

    rows, model = hidden_ref.shape
    local = q_ref.shape[1]
    one = Scatter(spot, p_ref, from_one, chip_one, landed_one, send_one, recv_one)
    outer = Scatter(spot, po_ref, from_out, chip_out, landed_out, send_out, recv_out)
    one.start_first()
    one.start_last()
    outer.start_first()
    outer.start_last()
    per = 2 + 2 * (len(lines) - 1)

    def chunks_of(x_ref, o_ref):
        nonlocal rest
        made = []
        wide = min(width, x_ref.shape[1])
        for start in range(0, x_ref.shape[1], wide):
            made.append(sum_chunk(lines, x_ref, o_ref, pl.ds(start, wide), rest[:per], rest[per], rest[per + 1]))
            rest = rest[per + 2 :]
        return made

    turns = Turns(chunks_of(gi_ref, si_ref) + chunks_of(go_ref, so_ref))
    one.cross()

    dk_acc[...] = jnp.zeros_like(dk_acc)
    dv_acc[...] = jnp.zeros_like(dv_acc)
    part = rows // PARTS
    to_across, to_sib, passed = [], [], []

    def block_part(owner, i):
        return gattn_ref.at[pl.ds(pl.multiple_of(owner * rows + i * part, part), part)]

    def back(values, grad_hat):
        normed, inverse = norm_parts(values)
        return inverse * (
            grad_hat
            - jnp.mean(grad_hat, axis=-1, keepdims=True)
            - normed * jnp.mean(grad_hat * normed, axis=-1, keepdims=True)
        )

    for i in range(PARTS):
        here = pl.ds(i * part, part)
        grad_second = one.result(i)
        gsec_ref[here, :] = grad_second
        grad_hidden = cot_ref[here, :].astype(F32) + back(hidden_ref[here, :], grad_second * gain_ref[1:2, :])
        ghid_ref[here, :] = grad_hidden
        gattn_ref[pl.ds(pl.multiple_of(me * rows + i * part, part), part), :] = grad_hidden.astype(BF16)
        ref = block_part(me, i)
        to_across.append(remote(ref, ref, gsend.at[i], grecv.at[i], (dp, across)))
        to_across[-1].start()
        to_sib.append(remote(ref, ref, gsend.at[PARTS + i], grecv.at[PARTS + i], (dp, sib)))
        to_sib[-1].start()
    turns.turn()
    outer.cross()

    heads = local // HDIM
    scale = HDIM ** (-0.5)
    lanes = lax.broadcasted_iota(jnp.int32, (rows, local), 1) // HDIM

    def attend(owner):
        block = pl.ds(pl.multiple_of(owner * rows, rows), rows)
        grad_att = dot(gattn_ref[block, :], w_out_ref[...], ((1,), (1,))).astype(BF16)
        query = q_ref[block, :]
        for h in range(heads):
            do_cat[pl.ds(h * rows, rows), :] = jnp.where(lanes == h, grad_att, jnp.zeros_like(grad_att))
            q_cat[pl.ds(h * rows, rows), :] = jnp.where(lanes == h, query, jnp.zeros_like(query))

        @pl.loop(0, heads)
        def _(h):
            at = pl.ds(pl.multiple_of(h * rows, rows), rows)
            scores = dot(k_ref[...], q_cat[at, :], ((1,), (1,)))
            probs = jnp.exp(scores * scale + (bias_ref[...] - log_ref[owner * heads + h]))
            grad_probs = dot(v_ref[...], do_cat[at, :], ((1,), (1,)))
            centre = jnp.sum(probs * grad_probs, axis=0, keepdims=True)
            grad_scores = (probs * (grad_probs - centre)).astype(BF16)
            p_scr[:, at] = probs.astype(BF16)
            ds_scr[:, at] = grad_scores
            head = pl.ds(pl.multiple_of(h * HDIM, HDIM), HDIM)
            dqt_ref[owner, head, :] = dot(kt_ref[head, :], grad_scores, ((1,), (0,)))

        dv_acc[...] += dot(p_scr[...], do_cat[...], ((1,), (0,)))
        dk_acc[...] += dot(ds_scr[...], q_cat[...], ((1,), (0,)))

    def pass_on(i):
        to_across[i].wait_recv()
        ref = block_part(across, i)
        passed.append(remote(ref, ref, gsend.at[2 * PARTS + i], grecv.at[2 * PARTS + i], (dp, sib)))
        passed[-1].start()

    attend(me)
    turns.turn()
    pass_on(0)
    pass_on(1)
    for copy in to_sib:
        copy.wait_recv()
    attend(sib)
    pass_on(2)
    pass_on(3)
    turns.turn()
    attend(across)
    turns.turn()
    for copy in passed:
        copy.wait_recv()
    attend(diag)
    turns.turn()

    dqkv_ref[:, pl.ds(local, local)] = (dk_acc[...] * scale).astype(BF16)
    dqkv_ref[:, pl.ds(2 * local, local)] = dv_acc[...].astype(BF16)
    total_ref = p_scr
    two = Scatter(spot, total_ref, from_two, chip_two, landed_two, send_two, recv_two)

    def total(owner):
        block = pl.ds(pl.multiple_of(owner * rows, rows), rows)
        grad_query = (dqt_ref[owner].T * scale).astype(BF16)
        dqkv_ref[block, pl.ds(0, local)] = grad_query
        total_ref[block, :] = (
            dot(grad_query, wq_ref[...], ((1,), (1,)))
            + dot(dqkv_ref[block, pl.ds(local, local)], wk_ref[...], ((1,), (1,)))
            + dot(dqkv_ref[block, pl.ds(2 * local, local)], wv_ref[...], ((1,), (1,)))
        ).astype(BF16)

    total(diag)
    two.start_first()
    total(across)
    two.cross()
    total(sib)
    two.start_last()
    total(me)
    turns.turn()

    grads_ref = ds_scr

    @pl.loop(0, model // rows)
    def _(i):
        at = pl.ds(pl.multiple_of(i * rows, rows), rows)
        grads_ref[at, pl.ds(0, 3 * local)] = dot(first_ref[:, at], dqkv_ref[...], ((0,), (0,))).astype(BF16)
        grads_ref[at, pl.ds(3 * local, local)] = dot(gattn_ref[:, at], att_ref[...], ((0,), (0,))).astype(BF16)

    for chunk in chunks_of(grads_ref, sa_ref):
        turns.add(chunk)
    turns.turn()

    def put(row, sums):
        for j in range(sums.shape[1] // 128):
            vec_ref[pl.ds(row + j, 1), :] = sums[:, j * 128 : (j + 1) * 128]

    vec_ref[...] = jnp.zeros_like(vec_ref)
    units = gb_ref.shape[0]
    per_row = model // 128
    sums = [jnp.zeros((1, model), F32) for _ in range(6)]
    for i in range(PARTS):
        here = pl.ds(i * part, part)
        grad_first = two.result(i)
        values = frames_ref[here, :].astype(F32)
        normed_one, _ = norm_parts(values)
        normed_two, _ = norm_parts(hidden_ref[here, :])
        grad_hidden = ghid_ref[here, :]
        grad_second = gsec_ref[here, :]
        fgrad_ref[here, :] = grad_hidden + back(values, grad_first * gain_ref[0:1, :])
        for k, block in enumerate(
            (
                grad_first * normed_one,
                grad_second * normed_two,
                grad_first,
                grad_second,
                grad_hidden,
                cot_ref[here, :].astype(F32),
            )
        ):
            sums[k] = sums[k] + column_sums(block)
    for k in range(6):
        put(k * per_row, sums[k])
    base = 6 * per_row
    shared = base
    near = [(dp, sib), (dp, across), (dp, diag)]
    vec_copies = [
        remote(vec_ref.at[pl.ds(0, shared)], vec_got.at[i], vec_send.at[i], vec_recv.at[i], device)
        for i, device in enumerate(near)
    ]
    for copy in vec_copies:
        copy.start()
    turns.turn()
    vec_ref[pl.ds(base, units), :] = gb_ref[...]
    put(base + units, column_sums(dqkv_ref[:, pl.ds(0, local)].astype(F32)))
    put(base + units + local // 128, column_sums(dqkv_ref[:, pl.ds(2 * local, local)].astype(F32)))
    for i in range(PARTS):
        here = pl.ds(i * part, part)
        out_ref[here, :] = (hidden_ref[here, :] + outer.result(i) + b_outer_ref[...]).astype(BF16)
    for copy in vec_copies:
        copy.wait_recv()
    every = vec_ref[pl.ds(0, shared), :] + vec_got[0] + vec_got[1] + vec_got[2]
    sections = pick_ref.shape[0]
    small_in[...] = jnp.zeros_like(small_in)
    table = 4 * per_row
    for k in range(sections):
        small_in[pl.ds(table * k, table), :] = (every[0:table] * pick_ref[k : k + 1, :]).astype(BF16)
    done = table * sections
    small_in[pl.ds(done, shared - table), :] = every[table:shared].astype(BF16)
    done += shared - table
    small_in[pl.ds(done, 16), :] = vec_ref[pl.ds(base, 16), :].astype(BF16)
    for chunk in chunks_of(small_in, small_ref):
        turns.add(chunk)
    turns.drain()
    one.finish()
    two.finish()
    outer.finish()
    for copy in to_across + to_sib + passed + vec_copies:
        copy.wait_send()


def late(count, width, cid, *operands):
    hidden, q, gi, go, pick = operands[2], operands[8], operands[19], operands[20], operands[22]
    rows, model = hidden.shape
    seq, local = q.shape
    heads = local // HDIM
    sems = chunk_sems(count)
    small_rows = -(-(4 * model // 128 * pick.shape[0] + 2 * model // 128 + 16) // (16 * count)) * 16 * count

    def dma(n):
        return [pltpu.SemaphoreType.DMA((n,))] * 2

    def scatter_scratch():
        return [
            pltpu.VMEM((2, rows, model), BF16),
            pltpu.VMEM((rows, model), BF16),
            pltpu.VMEM((rows, model), BF16),
        ] + dma(3 * PARTS)

    scratch = scatter_scratch() + scatter_scratch() + scatter_scratch()
    scratch += dma(3 * PARTS) + [pltpu.VMEM((3, 6 * model // 128, 128), F32)] + dma(3)
    scratch += [
        pltpu.VMEM((seq, model), BF16),
        pltpu.VMEM((rows, model), F32),
        pltpu.VMEM((rows, model), F32),
        pltpu.VMEM((seq, 3 * local), BF16),
        pltpu.VMEM((6 * model // 128 + 16, 128), F32),
        pltpu.VMEM((small_rows, 128), BF16),
        pltpu.VMEM((heads * rows, local), BF16),
        pltpu.VMEM((heads * rows, local), BF16),
        pltpu.VMEM((seq, heads * rows), BF16),
        pltpu.VMEM((seq, heads * rows), BF16),
        pltpu.VMEM((seq, local), F32),
        pltpu.VMEM((seq, local), F32),
        pltpu.VMEM((seq // rows, local, rows), F32),
    ]
    for grad in (gi, go, gi):
        for _ in range(0, grad.shape[1], width):
            scratch += chunk_scratch(count, grad.shape[0], width) + dma(sems)
    scratch += chunk_scratch(count, small_rows, 128) + dma(sems)
    shape = jax.ShapeDtypeStruct
    return pl.pallas_call(
        functools.partial(late_kernel, count, width),
        out_shape=[
            shape((rows, model), BF16),
            shape((rows, model), F32),
            shape(gi.shape, BF16),
            shape(go.shape, BF16),
            shape((model, 4 * local), BF16),
            shape((small_rows, 128), BF16),
        ],
        in_specs=whole_vmem(len(operands)),
        out_specs=whole_vmem(6),
        scratch_shapes=scratch,
        compiler_params=pltpu.CompilerParams(
            collective_id=cid, has_side_effects=True, vmem_limit_bytes=67043328
        ),
        name="late",
    )(*operands)


def normalize(row_block):
    centered = row_block - jnp.mean(row_block, axis=-1, keepdims=True)
    inverse = lax.rsqrt(jnp.mean(centered * centered, axis=-1, keepdims=True) + EPSILON)
    return (centered * inverse, inverse)


def exact_gelu(values):
    return jax.nn.gelu(values, approximate=False)


def split_heads(flat_rows):
    return flat_rows.reshape(-1, SEQ, flat_rows.shape[1] // HDIM, HDIM)


def dot(a, b, dims):
    return lax.dot_general(a, b, (dims, ((), ())), preferred_element_type=F32)


def masked_scores(query_block, keys_all, valid_keys, score_scale):
    scores = jnp.einsum("sqhe,skhe->shqk", query_block, keys_all, preferred_element_type=F32) * score_scale
    return jnp.where(valid_keys[:, None, None, :], scores, NEG_LARGE)


def attention_forward(queries, keys_all, values_all, valid_keys, score_scale, block_rows):
    pieces = []
    log_sums = []
    for offset in range(0, SEQ, block_rows):
        scores = masked_scores(queries[:, offset : offset + block_rows], keys_all, valid_keys, score_scale)
        highest = jnp.max(scores, axis=-1, keepdims=True)
        weights = jnp.exp(scores - highest)
        totals = jnp.sum(weights, axis=-1, keepdims=True)
        softmax_low = (weights / totals).astype(BF16)
        mixture = jnp.einsum("shqk,skhe->sqhe", softmax_low, values_all, preferred_element_type=F32)
        pieces.append(mixture.astype(BF16))
        log_sums.append((highest + jnp.log(totals))[..., 0])
    return (jnp.concatenate(pieces, axis=1), jnp.concatenate(log_sums, axis=2))


def body(
    dp_count,
    frames,
    cotangent,
    ada_gain,
    ada_shift,
    w_query,
    b_query,
    w_key,
    w_value,
    b_value,
    w_out,
    b_out,
    w_inner,
    b_inner,
    w_outer,
    b_outer,
    section_index,
    lengths,
    key_mask,
):
    rows_dev, width = frames.shape
    sections = ada_gain.shape[0]
    assert section_index.shape[0] == 1
    score_scale = HDIM ** (-0.5)
    block_rows = 512
    section = section_index[0] - 2
    gain = lax.dynamic_slice(ada_gain, (section, 0), (1, 2 * width))
    shift = lax.dynamic_slice(ada_shift, (section, 0), (1, 2 * width))
    pick = jnp.broadcast_to(
        (section == jnp.arange(sections, dtype=jnp.int32)).astype(F32)[:, None], (sections, 128)
    )
    spots = jnp.arange(SEQ, dtype=jnp.int32)
    valid_keys = (spots[None, :] < lengths[:, None]) & (key_mask.reshape(1, SEQ) > 0)
    inputs = frames.astype(F32)
    normed_one, inverse_one = normalize(inputs)
    first_low = (normed_one * gain[:, :width] + shift[:, :width]).astype(BF16)
    first_all = tensor_gather(first_low, 1)
    queries = (dot(first_all, w_query, ((1,), (0,))) + b_query).astype(BF16)
    keys_all = dot(first_all, w_key, ((1,), (0,))).astype(BF16)
    values_all = (dot(first_all, w_value, ((1,), (0,))) + b_value).astype(BF16)
    attended_heads, log_sums = attention_forward(
        split_heads(queries), split_heads(keys_all), split_heads(values_all), valid_keys, score_scale, block_rows
    )
    attended = attended_heads.reshape(queries.shape)
    hidden = inputs + tensor_scatter(dot(attended, w_out, ((1,), (0,))).astype(BF16), 2) + b_out
    normed_two, inverse_two = normalize(hidden)
    second_low = (normed_two * gain[:, width:] + shift[:, width:]).astype(BF16)
    second_all = tensor_gather(second_low, 3)
    grad_all = tensor_gather(cotangent, 4)
    inner_pre = dot(second_all, w_inner, ((1,), (0,))) + b_inner
    activated = exact_gelu(inner_pre).astype(BF16)
    outer_part = dot(activated, w_outer, ((1,), (0,))).astype(BF16)
    grad_w_outer = dot(activated, grad_all, ((0,), (0,))).astype(BF16)
    grad_activated = dot(grad_all, w_outer, ((1,), (1,)))
    unused_value, gelu_pull = jax.vjp(exact_gelu, inner_pre)
    grad_inner = gelu_pull(grad_activated)[0].astype(BF16)
    grad_w_inner = dot(second_all, grad_inner, ((0,), (0,))).astype(BF16)
    grad_b_inner = jnp.sum(grad_inner.astype(F32), axis=0)
    second_part = dot(grad_inner, w_inner, ((1,), (1,))).astype(BF16)
    bias_keys = jnp.broadcast_to(jnp.where(valid_keys[0], 0.0, NEG_LARGE)[:, None], (SEQ, rows_dev))
    heads_here = w_query.shape[1] // HDIM
    logs = log_sums.reshape(heads_here, SEQ // rows_dev, rows_dev).transpose(1, 0, 2)
    layer_out, frames_grad, sum_inner, sum_outer, sum_attn, small = late(
        dp_count,
        512,
        6,
        second_part,
        outer_part,
        hidden,
        frames,
        cotangent,
        gain.reshape(2, width),
        b_outer.reshape(1, width),
        w_out,
        queries,
        keys_all,
        keys_all.T,
        values_all,
        logs.reshape(-1, 1, rows_dev),
        bias_keys,
        w_query,
        w_key,
        w_value,
        first_all,
        attended,
        grad_w_inner,
        grad_w_outer,
        grad_b_inner.reshape(-1, 128),
        pick,
    )
    small = small.astype(F32)
    tables = small[: 32 * sections].reshape(sections, 2, 2 * width)
    shared = small[32 * sections : 32 * sections + 16].reshape(2, width)
    biases = small[32 * sections + 16 : 32 * sections + 32].reshape(-1)
    heads = w_query.shape[1]
    units = w_inner.shape[1]
    return (
        layer_out,
        frames_grad,
        tables[:, 0],
        tables[:, 1],
        sum_attn[:, :heads].astype(F32),
        biases[units : units + heads],
        sum_attn[:, heads : 2 * heads].astype(F32),
        sum_attn[:, 2 * heads : 3 * heads].astype(F32),
        biases[units + heads : units + 2 * heads],
        sum_attn[:, 3 * heads :].T.astype(F32),
        shared[0],
        sum_inner.astype(F32),
        biases[:units],
        sum_outer.astype(F32),
        shared[1],
    )


def solution(mesh):
    return jax.shard_map(
        functools.partial(body, mesh.shape["dp"]),
        mesh=mesh,
        in_specs=(
            P(("dp", "tensor"), None),
            P(("dp", "tensor"), None),
            P(),
            P(),
            P(None, "tensor"),
            P("tensor"),
            P(None, "tensor"),
            P(None, "tensor"),
            P("tensor"),
            P("tensor", None),
            P(),
            P(None, "tensor"),
            P("tensor"),
            P("tensor", None),
            P(),
            P("dp"),
            P("dp"),
            P("dp"),
        ),
        out_specs=(
            P(("dp", "tensor"), None),
            P(("dp", "tensor"), None),
            P(),
            P(),
            P(None, "tensor"),
            P("tensor"),
            P(None, "tensor"),
            P(None, "tensor"),
            P("tensor"),
            P("tensor", None),
            P(),
            P(None, "tensor"),
            P("tensor"),
            P("tensor", None),
            P(),
        ),
        check_vma=False,
    )
```

```python
import functools

import jax
import jax.numpy as jnp
from jax import lax
from jax.experimental import pallas as pl
from jax.experimental.pallas import tpu as pltpu
from jax.sharding import PartitionSpec as P

HDIM = 64
SEQ = 1024
EPSILON = 1e-05
NEG_LARGE = -1e30
F32 = jnp.float32
BF16 = jnp.bfloat16
MESH = pl.DeviceIdType.MESH
VMEM_LIMIT = 60 * 1024 * 1024


def places():
    dp = lax.axis_index("dp")
    me = lax.axis_index("tensor")
    sib = me + 1 - 2 * (me % 2)
    across = (me + 2) % 4
    diag = (sib + 2) % 4
    return dp, me, sib, across, diag


def greet(partners):
    barrier = pltpu.get_barrier_semaphore()
    for partner in partners:
        pl.semaphore_signal(barrier, inc=1, device_id=partner, device_id_type=MESH)
    pl.semaphore_wait(barrier, len(partners))


def remote(src, dst, send, recv, device):
    return pltpu.make_async_remote_copy(
        src_ref=src, dst_ref=dst, send_sem=send, recv_sem=recv, device_id=device, device_id_type=MESH
    )


def whole_vmem(count):
    return [pl.BlockSpec(memory_space=pltpu.VMEM)] * count


PARTS = 4


def dp_lines(count):
    sizes, limit = [], 2
    while count > 1:
        size = min(count, limit)
        sizes.append(size)
        count //= size
        limit *= 2
    return sizes


class Line:
    def __init__(self, size, stride, dp, me):
        self.size = size
        self.place = (dp // stride) % size
        self.right = (jnp.minimum(dp + stride, dp + (size - 1 - self.place) * stride), me)
        self.left = (jnp.maximum(dp - stride, dp - self.place * stride), me)
        self.pair = (dp + stride - 2 * stride * (dp // stride % 2), me)


def lines_of(count, dp, me):
    found, stride = [], 1
    for size in dp_lines(count):
        found.append(Line(size, stride, dp, me))
        stride *= size
    return found


def chunk_sems(count):
    sizes = dp_lines(count)
    return 1 + sizes[1] + sum(4 * size for size in sizes[1:])


def chunk_scratch(count, rows, width):
    sizes = dp_lines(count)
    shapes = [pltpu.VMEM((rows // 2, width), BF16), pltpu.VMEM((rows // 2, width), BF16)]
    part = rows // 2
    for size in sizes[1:]:
        part //= size
        shapes += [pltpu.VMEM((size - 1, part, width), BF16)] * 2
    return shapes


def sum_chunk(lines, x_ref, o_ref, columns, scratch, send, recv):
    rows = x_ref.shape[0]
    got, own = scratch[0], scratch[1]
    buffers = [scratch[2 + 2 * i : 4 + 2 * i] for i in range(len(lines) - 1)]
    pair = lines[0]
    half = rows // 2
    started = []
    used = [0]

    def slots(count):
        used[0] += count
        return used[0] - count

    def go(copy, condition=None):
        if condition is None:
            copy.start()
        else:
            pl.when(condition)(lambda: copy.start())
        started.append((copy, condition))

    def when(condition, body):
        pl.when(condition)(body)

    mine = pl.multiple_of(pair.place * half, half)
    other = pl.multiple_of(half - pair.place * half, half)
    slot = slots(1)
    first = remote(x_ref.at[pl.ds(other, half), columns], got, send.at[slot], recv.at[slot], pair.pair)
    go(first)
    yield
    first.wait_recv()
    own[...] = (x_ref[pl.ds(mine, half), columns].astype(F32) + got[...].astype(F32)).astype(BF16)
    base = 0
    size_now = half
    for line, (to_right, to_left) in zip(lines[1:], buffers):
        n, z = line.size, line.place
        part = size_now // n
        right_slot, left_slot = slots(n), slots(n)
        bases = base

        def piece(o, part=part, bases=bases):
            return pl.ds(pl.multiple_of(bases + o * part, part), part)

        for j in range(n - 1, 0, -1):
            for way in (0, 1):
                o = z + j if way == 0 else z - j
                inside = (o < n) if way == 0 else (o >= 0)
                buffer = to_right if way == 0 else to_left
                at_end = (z == 0) if way == 0 else (z == n - 1)
                slot = (right_slot if way == 0 else left_slot) + jnp.clip(o, 0, n - 1)
                o = jnp.clip(o, 0, n - 1)
                at = jnp.clip(o - 1 + way, 0, n - 2)
                there = line.right if way == 0 else line.left
                copy = remote(own.at[piece(o)], buffer.at[at], send.at[slot], recv.at[slot], there)
                onward = remote(buffer.at[at], buffer.at[at], send.at[slot], recv.at[slot], there)
                go(copy, inside & at_end)

                def pass_on(buffer=buffer, o=o, at=at, onward=onward, piece=piece):
                    onward.wait_recv()
                    buffer[at] = (buffer[at].astype(F32) + own[piece(o), :].astype(F32)).astype(BF16)
                    onward.start()

                when(inside & jnp.logical_not(at_end), pass_on)
                started.append((onward, inside & jnp.logical_not(at_end)))
            yield

        def take(buffer, slot, at, line=line, piece=piece, z=z):
            remote(buffer.at[at], buffer.at[at], send.at[slot + z], recv.at[slot + z], line.right).wait_recv()
            own[piece(z), :] = (own[piece(z), :].astype(F32) + buffer[at].astype(F32)).astype(BF16)

        when(z > 0, functools.partial(take, to_right, right_slot, jnp.maximum(z - 1, 0)))
        when(z < n - 1, functools.partial(take, to_left, left_slot, jnp.minimum(z, n - 2)))
        base = bases + z * part
        size_now = part
    final = pl.ds(pl.multiple_of(mine + base, size_now), size_now)
    o_ref[final, columns] = own[pl.ds(pl.multiple_of(base, size_now), size_now), :]
    region = mine + base
    for level in range(len(lines) - 1, 0, -1):
        line = lines[level]
        n, z = line.size, line.place
        part = size_now
        base_region = region - z * part
        right_slot, left_slot = slots(n), slots(n)
        pair_slot = slots(n) if level == 1 else None

        def piece(o, part=part, base_region=base_region):
            return pl.ds(pl.multiple_of(base_region + o * part, part), part)

        def copy_of(o, slot, there, piece=piece):
            ref = o_ref.at[piece(o), columns]
            return remote(ref, ref, send.at[slot + o], recv.at[slot + o], there)

        go(copy_of(z, right_slot, line.right), z < n - 1)
        go(copy_of(z, left_slot, line.left), z > 0)
        if level == 1:
            go(copy_of(z, pair_slot, pair.pair))
        yield
        for j in range(1, n):
            for way in (0, 1):
                o = z - j if way == 0 else z + j
                inside = (o >= 0) if way == 0 else (o < n)
                goes_on = (z < n - 1) if way == 0 else (z > 0)
                o = jnp.clip(o, 0, n - 1)
                slot = right_slot if way == 0 else left_slot
                there = line.right if way == 0 else line.left
                copy = copy_of(o, slot, there)
                when(inside, lambda copy=copy: copy.wait_recv())
                go(copy, inside & goes_on)
                if level == 1:
                    go(copy_of(o, pair_slot, pair.pair), inside)
            yield
        region = base_region
        size_now = part * n
        if level == 1:
            for o in range(n):
                ref = o_ref.at[pl.ds(pl.multiple_of(other + o * part, part), part), columns]
                remote(ref, ref, send.at[pair_slot + o], recv.at[pair_slot + o], pair.pair).wait_recv()
    for copy, condition in started:
        if condition is None:
            copy.wait_send()
        else:
            when(condition, lambda copy=copy: copy.wait_send())


class Turns:
    def __init__(self, generators):
        self.waiting = list(generators)
        self.running = []
        for generator in self.waiting:
            next(generator)

    def add(self, generator):
        next(generator)
        self.waiting.append(generator)

    def turn(self):
        if self.waiting:
            self.running.append(self.waiting.pop(0))
        still = []
        for generator in self.running:
            try:
                next(generator)
                still.append(generator)
            except StopIteration:
                pass
        self.running = still

    def drain(self):
        while self.waiting or self.running:
            self.turn()


class Scatter:
    def __init__(self, spot, p_ref, from_sib, chip_sum, landed, send, recv):
        self.dp, self.me, self.sib, self.across, self.diag = spot
        self.rows = p_ref.shape[0] // 4
        self.part = self.rows // PARTS
        self.p_ref, self.from_sib, self.chip_sum, self.landed = p_ref, from_sib, chip_sum, landed

        def near(owner, which, i):
            slot = which * PARTS + i
            return remote(
                p_ref.at[self.at(owner, i)],
                from_sib.at[which, self.here(i)],
                send.at[slot],
                recv.at[slot],
                (self.dp, self.sib),
            )

        self.first = [near(self.diag, 0, i) for i in range(PARTS)]
        self.last = [near(self.sib, 1, i) for i in range(PARTS)]
        self.crossing = [
            remote(
                chip_sum.at[self.here(i)],
                landed.at[self.here(i)],
                send.at[2 * PARTS + i],
                recv.at[2 * PARTS + i],
                (self.dp, self.across),
            )
            for i in range(PARTS)
        ]

    def here(self, i):
        return pl.ds(i * self.part, self.part)

    def at(self, owner, i):
        return pl.ds(pl.multiple_of(owner * self.rows + i * self.part, self.part), self.part)

    def start_first(self):
        for copy in self.first:
            copy.start()

    def start_last(self):
        for copy in self.last:
            copy.start()

    def cross(self):
        for i in range(PARTS):
            self.first[i].wait_recv()
            self.chip_sum[self.here(i), :] = (
                self.p_ref[self.at(self.across, i), :].astype(F32) + self.from_sib[0, self.here(i), :].astype(F32)
            ).astype(BF16)
            self.crossing[i].start()

    def result(self, i):
        self.last[i].wait_recv()
        total = self.p_ref[self.at(self.me, i), :].astype(F32) + self.from_sib[1, self.here(i), :].astype(F32)
        self.crossing[i].wait_recv()
        return total + self.landed[self.here(i), :].astype(F32)

    def finish(self):
        for copy in self.first + self.last + self.crossing:
            copy.wait_send()


class Gather:
    def __init__(self, spot, all_ref, send, recv):
        self.dp, self.me, self.sib, self.across, self.diag = spot
        self.rows = all_ref.shape[0] // 4
        self.part = self.rows // PARTS

        def copy(owner, i, slot, device):
            ref = all_ref.at[self.at(owner, i)]
            return remote(ref, ref, send.at[slot], recv.at[slot], (self.dp, device))

        self.to_across = [copy(self.me, i, i, self.across) for i in range(PARTS)]
        self.to_sib = [copy(self.me, i, PARTS + i, self.sib) for i in range(PARTS)]
        self.passed = [copy(self.across, i, 2 * PARTS + i, self.sib) for i in range(PARTS)]

    def at(self, owner, i):
        return pl.ds(pl.multiple_of(owner * self.rows + i * self.part, self.part), self.part)

    def start(self, i):
        self.to_across[i].start()
        self.to_sib[i].start()

    def pass_on(self, i):
        self.to_across[i].wait_recv()
        self.passed[i].start()

    def wait_sib(self):
        for copy in self.to_sib:
            copy.wait_recv()

    def wait_diag(self):
        for copy in self.passed:
            copy.wait_recv()

    def finish(self):
        for copy in self.to_across + self.to_sib + self.passed:
            copy.wait_send()


def norm_parts(block):
    centered = block - jnp.mean(block, axis=-1, keepdims=True)
    inverse = lax.rsqrt(jnp.mean(centered * centered, axis=-1, keepdims=True) + EPSILON)
    return centered * inverse, inverse


def column_sums(block):
    return jnp.sum(block, axis=0, keepdims=True)


def late_kernel(count, width, *refs):
    p_ref, po_ref, hidden_ref, frames_ref, cot_ref, gain_ref, b_outer_ref = refs[:7]
    w_out_ref, q_ref, k_ref, kt_ref, v_ref, log_ref, bias_ref = refs[7:14]
    wq_ref, wk_ref, wv_ref, first_ref, att_ref, gi_ref, go_ref, gb_ref, pick_ref = refs[14:23]
    out_ref, fgrad_ref, si_ref, so_ref, sa_ref, small_ref = refs[23:29]
    rest = refs[29:]
    from_one, chip_one, landed_one, send_one, recv_one = rest[:5]
    from_two, chip_two, landed_two, send_two, recv_two = rest[5:10]
    from_out, chip_out, landed_out, send_out, recv_out = rest[10:15]
    gsend, grecv, vec_got, vec_send, vec_recv = rest[15:20]
    gattn_ref, gsec_ref, ghid_ref, dqkv_ref, vec_ref, small_in = rest[20:26]
    do_cat, q_cat, p_scr, ds_scr, dk_acc, dv_acc, dqt_ref = rest[26:33]
    rest = rest[33:]
    spot = places()
    dp, me, sib, across, diag = spot
    lines = lines_of(count, dp, me)
    barrier = pltpu.get_barrier_semaphore()
    for partner in [(dp, sib), (dp, across), (dp, diag), lines[0].pair]:
        pl.semaphore_signal(barrier, inc=1, device_id=partner, device_id_type=MESH)
    waits = 4
    for line in lines[1:]:
        has_right = line.place < line.size - 1
        has_left = line.place > 0
        for partner, has in ((line.right, has_right), (line.left, has_left)):
            pl.when(has)(
                lambda partner=partner: pl.semaphore_signal(
                    barrier, inc=1, device_id=partner, device_id_type=MESH
                )
            )
        waits = waits + has_right.astype(jnp.int32) + has_left.astype(jnp.int32)
    pl.semaphore_wait(barrier, waits)

    rows, model = hidden_ref.shape
    local = q_ref.shape[1]
    one = Scatter(spot, p_ref, from_one, chip_one, landed_one, send_one, recv_one)
    outer = Scatter(spot, po_ref, from_out, chip_out, landed_out, send_out, recv_out)
    one.start_first()
    one.start_last()
    outer.start_first()
    outer.start_last()
    per = 2 + 2 * (len(lines) - 1)

    def chunks_of(x_ref, o_ref):
        nonlocal rest
        made = []
        wide = min(width, x_ref.shape[1])
        for start in range(0, x_ref.shape[1], wide):
            made.append(sum_chunk(lines, x_ref, o_ref, pl.ds(start, wide), rest[:per], rest[per], rest[per + 1]))
            rest = rest[per + 2 :]
        return made

    turns = Turns(chunks_of(gi_ref, si_ref) + chunks_of(go_ref, so_ref))
    one.cross()

    dk_acc[...] = jnp.zeros_like(dk_acc)
    dv_acc[...] = jnp.zeros_like(dv_acc)
    part = rows // PARTS
    to_across, to_sib, passed = [], [], []

    def block_part(owner, i):
        return gattn_ref.at[pl.ds(pl.multiple_of(owner * rows + i * part, part), part)]

    def back(values, grad_hat):
        normed, inverse = norm_parts(values)
        return inverse * (
            grad_hat
            - jnp.mean(grad_hat, axis=-1, keepdims=True)
            - normed * jnp.mean(grad_hat * normed, axis=-1, keepdims=True)
        )

    for i in range(PARTS):
        here = pl.ds(i * part, part)
        grad_second = one.result(i)
        gsec_ref[here, :] = grad_second
        grad_hidden = cot_ref[here, :].astype(F32) + back(hidden_ref[here, :], grad_second * gain_ref[1:2, :])
        ghid_ref[here, :] = grad_hidden
        gattn_ref[pl.ds(pl.multiple_of(me * rows + i * part, part), part), :] = grad_hidden.astype(BF16)
        ref = block_part(me, i)
        to_across.append(remote(ref, ref, gsend.at[i], grecv.at[i], (dp, across)))
        to_across[-1].start()
        to_sib.append(remote(ref, ref, gsend.at[PARTS + i], grecv.at[PARTS + i], (dp, sib)))
        to_sib[-1].start()
    turns.turn()
    outer.cross()

    heads = local // HDIM
    scale = HDIM ** (-0.5)
    lanes = lax.broadcasted_iota(jnp.int32, (rows, local), 1) // HDIM

    def attend(owner):
        block = pl.ds(pl.multiple_of(owner * rows, rows), rows)
        grad_att = dot(gattn_ref[block, :], w_out_ref[...], ((1,), (1,))).astype(BF16)
        query = q_ref[block, :]
        for h in range(heads):
            do_cat[pl.ds(h * rows, rows), :] = jnp.where(lanes == h, grad_att, jnp.zeros_like(grad_att))
            q_cat[pl.ds(h * rows, rows), :] = jnp.where(lanes == h, query, jnp.zeros_like(query))

        @pl.loop(0, heads)
        def _(h):
            at = pl.ds(pl.multiple_of(h * rows, rows), rows)
            scores = dot(k_ref[...], q_cat[at, :], ((1,), (1,)))
            probs = jnp.exp(scores * scale + (bias_ref[...] - log_ref[owner * heads + h]))
            grad_probs = dot(v_ref[...], do_cat[at, :], ((1,), (1,)))
            centre = jnp.sum(probs * grad_probs, axis=0, keepdims=True)
            grad_scores = (probs * (grad_probs - centre)).astype(BF16)
            p_scr[:, at] = probs.astype(BF16)
            ds_scr[:, at] = grad_scores
            head = pl.ds(pl.multiple_of(h * HDIM, HDIM), HDIM)
            dqt_ref[owner, head, :] = dot(kt_ref[head, :], grad_scores, ((1,), (0,)))

        dv_acc[...] += dot(p_scr[...], do_cat[...], ((1,), (0,)))
        dk_acc[...] += dot(ds_scr[...], q_cat[...], ((1,), (0,)))

    def pass_on(i):
        to_across[i].wait_recv()
        ref = block_part(across, i)
        passed.append(remote(ref, ref, gsend.at[2 * PARTS + i], grecv.at[2 * PARTS + i], (dp, sib)))
        passed[-1].start()

    attend(me)
    turns.turn()
    pass_on(0)
    pass_on(1)
    for copy in to_sib:
        copy.wait_recv()
    attend(sib)
    pass_on(2)
    pass_on(3)
    turns.turn()
    attend(across)
    turns.turn()
    for copy in passed:
        copy.wait_recv()
    attend(diag)
    turns.turn()

    dqkv_ref[:, pl.ds(local, local)] = (dk_acc[...] * scale).astype(BF16)
    dqkv_ref[:, pl.ds(2 * local, local)] = dv_acc[...].astype(BF16)
    total_ref = p_scr
    two = Scatter(spot, total_ref, from_two, chip_two, landed_two, send_two, recv_two)

    def total(owner):
        block = pl.ds(pl.multiple_of(owner * rows, rows), rows)
        grad_query = (dqt_ref[owner].T * scale).astype(BF16)
        dqkv_ref[block, pl.ds(0, local)] = grad_query
        total_ref[block, :] = (
            dot(grad_query, wq_ref[...], ((1,), (1,)))
            + dot(dqkv_ref[block, pl.ds(local, local)], wk_ref[...], ((1,), (1,)))
            + dot(dqkv_ref[block, pl.ds(2 * local, local)], wv_ref[...], ((1,), (1,)))
        ).astype(BF16)

    total(diag)
    two.start_first()
    total(across)
    two.cross()
    total(sib)
    two.start_last()
    total(me)
    turns.turn()

    grads_ref = ds_scr

    @pl.loop(0, model // rows)
    def _(i):
        at = pl.ds(pl.multiple_of(i * rows, rows), rows)
        grads_ref[at, pl.ds(0, 3 * local)] = dot(first_ref[:, at], dqkv_ref[...], ((0,), (0,))).astype(BF16)
        grads_ref[at, pl.ds(3 * local, local)] = dot(gattn_ref[:, at], att_ref[...], ((0,), (0,))).astype(BF16)

    for chunk in chunks_of(grads_ref, sa_ref):
        turns.add(chunk)
    turns.turn()

    def put(row, sums):
        for j in range(sums.shape[1] // 128):
            vec_ref[pl.ds(row + j, 1), :] = sums[:, j * 128 : (j + 1) * 128]

    vec_ref[...] = jnp.zeros_like(vec_ref)
    units = gb_ref.shape[0]
    per_row = model // 128
    sums = [jnp.zeros((1, model), F32) for _ in range(6)]
    for i in range(PARTS):
        here = pl.ds(i * part, part)
        grad_first = two.result(i)
        values = frames_ref[here, :].astype(F32)
        normed_one, _ = norm_parts(values)
        normed_two, _ = norm_parts(hidden_ref[here, :])
        grad_hidden = ghid_ref[here, :]
        grad_second = gsec_ref[here, :]
        fgrad_ref[here, :] = grad_hidden + back(values, grad_first * gain_ref[0:1, :])
        for k, block in enumerate(
            (
                grad_first * normed_one,
                grad_second * normed_two,
                grad_first,
                grad_second,
                grad_hidden,
                cot_ref[here, :].astype(F32),
            )
        ):
            sums[k] = sums[k] + column_sums(block)
    for k in range(6):
        put(k * per_row, sums[k])
    base = 6 * per_row
    shared = base
    near = [(dp, sib), (dp, across), (dp, diag)]
    vec_copies = [
        remote(vec_ref.at[pl.ds(0, shared)], vec_got.at[i], vec_send.at[i], vec_recv.at[i], device)
        for i, device in enumerate(near)
    ]
    for copy in vec_copies:
        copy.start()
    turns.turn()
    vec_ref[pl.ds(base, units), :] = gb_ref[...]
    put(base + units, column_sums(dqkv_ref[:, pl.ds(0, local)].astype(F32)))
    put(base + units + local // 128, column_sums(dqkv_ref[:, pl.ds(2 * local, local)].astype(F32)))
    for i in range(PARTS):
        here = pl.ds(i * part, part)
        out_ref[here, :] = (hidden_ref[here, :] + outer.result(i) + b_outer_ref[...]).astype(BF16)
    for copy in vec_copies:
        copy.wait_recv()
    every = vec_ref[pl.ds(0, shared), :] + vec_got[0] + vec_got[1] + vec_got[2]
    sections = pick_ref.shape[0]
    small_in[...] = jnp.zeros_like(small_in)
    table = 4 * per_row
    for k in range(sections):
        small_in[pl.ds(table * k, table), :] = (every[0:table] * pick_ref[k : k + 1, :]).astype(BF16)
    done = table * sections
    small_in[pl.ds(done, shared - table), :] = every[table:shared].astype(BF16)
    done += shared - table
    small_in[pl.ds(done, 16), :] = vec_ref[pl.ds(base, 16), :].astype(BF16)
    for chunk in chunks_of(small_in, small_ref):
        turns.add(chunk)
    turns.drain()
    one.finish()
    two.finish()
    outer.finish()
    for copy in to_across + to_sib + passed + vec_copies:
        copy.wait_send()


def late(count, width, cid, *operands):
    hidden, q, gi, go, pick = operands[2], operands[8], operands[19], operands[20], operands[22]
    rows, model = hidden.shape
    seq, local = q.shape
    heads = local // HDIM
    sems = chunk_sems(count)
    small_rows = -(-(4 * model // 128 * pick.shape[0] + 2 * model // 128 + 16) // (16 * count)) * 16 * count

    def dma(n):
        return [pltpu.SemaphoreType.DMA((n,))] * 2

    def scatter_scratch():
        return [
            pltpu.VMEM((2, rows, model), BF16),
            pltpu.VMEM((rows, model), BF16),
            pltpu.VMEM((rows, model), BF16),
        ] + dma(3 * PARTS)

    scratch = scatter_scratch() + scatter_scratch() + scatter_scratch()
    scratch += dma(3 * PARTS) + [pltpu.VMEM((3, 6 * model // 128, 128), F32)] + dma(3)
    scratch += [
        pltpu.VMEM((seq, model), BF16),
        pltpu.VMEM((rows, model), F32),
        pltpu.VMEM((rows, model), F32),
        pltpu.VMEM((seq, 3 * local), BF16),
        pltpu.VMEM((6 * model // 128 + 16, 128), F32),
        pltpu.VMEM((small_rows, 128), BF16),
        pltpu.VMEM((heads * rows, local), BF16),
        pltpu.VMEM((heads * rows, local), BF16),
        pltpu.VMEM((seq, heads * rows), BF16),
        pltpu.VMEM((seq, heads * rows), BF16),
        pltpu.VMEM((seq, local), F32),
        pltpu.VMEM((seq, local), F32),
        pltpu.VMEM((seq // rows, local, rows), F32),
    ]
    for grad in (gi, go, gi):
        for _ in range(0, grad.shape[1], width):
            scratch += chunk_scratch(count, grad.shape[0], width) + dma(sems)
    scratch += chunk_scratch(count, small_rows, 128) + dma(sems)
    shape = jax.ShapeDtypeStruct
    return pl.pallas_call(
        functools.partial(late_kernel, count, width),
        out_shape=[
            shape((rows, model), BF16),
            shape((rows, model), F32),
            shape(gi.shape, BF16),
            shape(go.shape, BF16),
            shape((model, 4 * local), BF16),
            shape((small_rows, 128), BF16),
        ],
        in_specs=whole_vmem(len(operands)),
        out_specs=whole_vmem(6),
        scratch_shapes=scratch,
        compiler_params=pltpu.CompilerParams(
            collective_id=cid, has_side_effects=True, vmem_limit_bytes=67043328
        ),
        name="late",
    )(*operands)


def front_kernel(*refs):
    frames_ref, cot_ref, gain_ref, shift_ref, wq_ref, bq_ref, wk_ref, wv_ref, bv_ref = refs[:9]
    bias_ref, w_out_ref, b_out_ref = refs[9:12]
    first_ref, call_ref, q_ref, k_ref, kt_ref, v_ref, log_ref, att_ref, hidden_ref, second_ref = refs[12:22]
    total_ref, vt_ref, q_cat, att_t, from_sib, chip_sum, landed = refs[22:29]
    ssend, srecv, asend, arecv, csend, crecv, bsend, brecv = refs[29:]
    spot = places()
    dp, me, sib, across, diag = spot
    greet([(dp, sib), (dp, across)])
    rows = frames_ref.shape[0]
    part = rows // PARTS
    local = q_ref.shape[1]
    heads = local // HDIM
    scale = HDIM ** (-0.5)
    firsts = Gather(spot, first_ref, asend, arecv)
    cots = Gather(spot, call_ref, csend, crecv)
    seconds = Gather(spot, second_ref, bsend, brecv)
    for i in range(PARTS):
        here = pl.ds(i * part, part)
        normed, _ = norm_parts(frames_ref[here, :].astype(F32))
        first_ref[firsts.at(me, i), :] = (normed * gain_ref[0:1, :] + shift_ref[0:1, :]).astype(BF16)
        firsts.start(i)
    for i in range(PARTS):
        call_ref[cots.at(me, i), :] = cot_ref[pl.ds(i * part, part), :]
        cots.start(i)

    def project(owner):
        block = pl.ds(pl.multiple_of(owner * rows, rows), rows)
        x = first_ref[block, :]
        q_ref[block, :] = (dot(x, wq_ref[...], ((1,), (0,))) + bq_ref[...]).astype(BF16)
        keys = dot(x, wk_ref[...], ((1,), (0,)))
        k_ref[block, :] = keys.astype(BF16)
        kt_ref[:, block] = keys.T.astype(BF16)
        values = dot(x, wv_ref[...], ((1,), (0,))) + bv_ref[...]
        v_ref[block, :] = values.astype(BF16)
        vt_ref[:, block] = values.T.astype(BF16)

    project(me)
    firsts.wait_sib()
    firsts.pass_on(0)
    firsts.pass_on(1)
    project(sib)
    firsts.pass_on(2)
    firsts.pass_on(3)
    project(across)
    firsts.wait_diag()
    project(diag)

    lanes = lax.broadcasted_iota(jnp.int32, (rows, local), 1) // HDIM

    def attend(owner):
        block = pl.ds(pl.multiple_of(owner * rows, rows), rows)
        query = q_ref[block, :]
        for h in range(heads):
            q_cat[pl.ds(h * rows, rows), :] = jnp.where(lanes == h, query, jnp.zeros_like(query))

        @pl.loop(0, heads, step=2)
        def _(pair):
            for h in (pair, pair + 1):
                at = pl.ds(pl.multiple_of(h * rows, rows), rows)
                scores = dot(k_ref[...], q_cat[at, :], ((1,), (1,))) * scale + bias_ref[...]
                highest = jnp.max(scores, axis=0, keepdims=True)
                weights = jnp.exp(scores - highest)
                sums = jnp.sum(weights, axis=0, keepdims=True)
                low = (weights * (1.0 / sums)).astype(BF16)
                head = pl.ds(pl.multiple_of(h * HDIM, HDIM), HDIM)
                att_t[head, :] = dot(vt_ref[head, :], low, ((1,), (0,)))
                log_ref[owner * heads + h] = highest + jnp.log(sums)

        attended = att_t[...].T.astype(BF16)
        att_ref[block, :] = attended
        total_ref[block, :] = dot(attended, w_out_ref[...], ((1,), (0,))).astype(BF16)

    sums = Scatter(spot, total_ref, from_sib, chip_sum, landed, ssend, srecv)
    attend(diag)
    sums.start_first()
    attend(across)
    sums.cross()
    attend(sib)
    sums.start_last()
    attend(me)
    for i in range(PARTS):
        here = pl.ds(i * part, part)
        hidden = frames_ref[here, :].astype(F32) + sums.result(i) + b_out_ref[...]
        hidden_ref[here, :] = hidden
        normed, _ = norm_parts(hidden)
        second_ref[seconds.at(me, i), :] = (normed * gain_ref[1:2, :] + shift_ref[1:2, :]).astype(BF16)
        seconds.start(i)
    for i in range(PARTS):
        cots.pass_on(i)
    for i in range(PARTS):
        seconds.pass_on(i)
    cots.wait_sib()
    cots.wait_diag()
    seconds.wait_sib()
    seconds.wait_diag()
    firsts.finish()
    cots.finish()
    sums.finish()
    seconds.finish()


def front(cid, *operands):
    frames, wq = operands[0], operands[4]
    rows, model = frames.shape
    local = wq.shape[1]
    heads = local // HDIM
    shape = jax.ShapeDtypeStruct
    return pl.pallas_call(
        front_kernel,
        out_shape=[
            shape((4 * rows, model), BF16),
            shape((4 * rows, model), BF16),
            shape((4 * rows, local), BF16),
            shape((4 * rows, local), BF16),
            shape((local, 4 * rows), BF16),
            shape((4 * rows, local), BF16),
            shape((4 * heads, 1, rows), F32),
            shape((4 * rows, local), BF16),
            shape((rows, model), F32),
            shape((4 * rows, model), BF16),
        ],
        in_specs=whole_vmem(len(operands)),
        out_specs=whole_vmem(10),
        scratch_shapes=[
            pltpu.VMEM((4 * rows, model), BF16),
            pltpu.VMEM((local, 4 * rows), BF16),
            pltpu.VMEM((heads * rows, local), BF16),
            pltpu.VMEM((local, rows), F32),
            pltpu.VMEM((2, rows, model), BF16),
            pltpu.VMEM((rows, model), BF16),
            pltpu.VMEM((rows, model), BF16),
        ]
        + [pltpu.SemaphoreType.DMA((3 * PARTS,))] * 8,
        compiler_params=pltpu.CompilerParams(
            collective_id=cid, has_side_effects=True, vmem_limit_bytes=VMEM_LIMIT
        ),
        name="front",
    )(*operands)


def exact_gelu(values):
    return jax.nn.gelu(values, approximate=False)


def dot(a, b, dims):
    return lax.dot_general(a, b, (dims, ((), ())), preferred_element_type=F32)


def body(
    dp_count,
    frames,
    cotangent,
    ada_gain,
    ada_shift,
    w_query,
    b_query,
    w_key,
    w_value,
    b_value,
    w_out,
    b_out,
    w_inner,
    b_inner,
    w_outer,
    b_outer,
    section_index,
    lengths,
    key_mask,
):
    rows_dev, width = frames.shape
    sections = ada_gain.shape[0]
    assert section_index.shape[0] == 1
    section = section_index[0] - 2
    gain = lax.dynamic_slice(ada_gain, (section, 0), (1, 2 * width))
    shift = lax.dynamic_slice(ada_shift, (section, 0), (1, 2 * width))
    pick = jnp.broadcast_to(
        (section == jnp.arange(sections, dtype=jnp.int32)).astype(F32)[:, None], (sections, 128)
    )
    spots = jnp.arange(SEQ, dtype=jnp.int32)
    valid_keys = (spots[None, :] < lengths[:, None]) & (key_mask.reshape(1, SEQ) > 0)
    bias_keys = jnp.broadcast_to(jnp.where(valid_keys[0], 0.0, NEG_LARGE)[:, None], (SEQ, rows_dev))
    first_all, grad_all, queries, keys_all, keys_turned, values_all, logs, attended, hidden, second_all = front(
        1,
        frames,
        cotangent,
        gain.reshape(2, width),
        shift.reshape(2, width),
        w_query,
        b_query.reshape(1, -1),
        w_key,
        w_value,
        b_value.reshape(1, -1),
        bias_keys,
        w_out,
        b_out.reshape(1, width),
    )
    inner_pre = dot(second_all, w_inner, ((1,), (0,))) + b_inner
    activated = exact_gelu(inner_pre).astype(BF16)
    outer_part = dot(activated, w_outer, ((1,), (0,))).astype(BF16)
    grad_w_outer = dot(activated, grad_all, ((0,), (0,))).astype(BF16)
    grad_activated = dot(grad_all, w_outer, ((1,), (1,)))
    unused_value, gelu_pull = jax.vjp(exact_gelu, inner_pre)
    grad_inner = gelu_pull(grad_activated)[0].astype(BF16)
    grad_w_inner = dot(second_all, grad_inner, ((0,), (0,))).astype(BF16)
    grad_b_inner = jnp.sum(grad_inner.astype(F32), axis=0)
    second_part = dot(grad_inner, w_inner, ((1,), (1,))).astype(BF16)
    layer_out, frames_grad, sum_inner, sum_outer, sum_attn, small = late(
        dp_count,
        512,
        6,
        second_part,
        outer_part,
        hidden,
        frames,
        cotangent,
        gain.reshape(2, width),
        b_outer.reshape(1, width),
        w_out,
        queries,
        keys_all,
        keys_turned,
        values_all,
        logs,
        bias_keys,
        w_query,
        w_key,
        w_value,
        first_all,
        attended,
        grad_w_inner,
        grad_w_outer,
        grad_b_inner.reshape(-1, 128),
        pick,
    )
    small = small.astype(F32)
    tables = small[: 32 * sections].reshape(sections, 2, 2 * width)
    shared = small[32 * sections : 32 * sections + 16].reshape(2, width)
    biases = small[32 * sections + 16 : 32 * sections + 32].reshape(-1)
    heads = w_query.shape[1]
    units = w_inner.shape[1]
    return (
        layer_out,
        frames_grad,
        tables[:, 0],
        tables[:, 1],
        sum_attn[:, :heads].astype(F32),
        biases[units : units + heads],
        sum_attn[:, heads : 2 * heads].astype(F32),
        sum_attn[:, 2 * heads : 3 * heads].astype(F32),
        biases[units + heads : units + 2 * heads],
        sum_attn[:, 3 * heads :].T.astype(F32),
        shared[0],
        sum_inner.astype(F32),
        biases[:units],
        sum_outer.astype(F32),
        shared[1],
    )


def solution(mesh):
    return jax.shard_map(
        functools.partial(body, mesh.shape["dp"]),
        mesh=mesh,
        in_specs=(
            P(("dp", "tensor"), None),
            P(("dp", "tensor"), None),
            P(),
            P(),
            P(None, "tensor"),
            P("tensor"),
            P(None, "tensor"),
            P(None, "tensor"),
            P("tensor"),
            P("tensor", None),
            P(),
            P(None, "tensor"),
            P("tensor"),
            P("tensor", None),
            P(),
            P("dp"),
            P("dp"),
            P("dp"),
        ),
        out_specs=(
            P(("dp", "tensor"), None),
            P(("dp", "tensor"), None),
            P(),
            P(),
            P(None, "tensor"),
            P("tensor"),
            P(None, "tensor"),
            P(None, "tensor"),
            P("tensor"),
            P("tensor", None),
            P(),
            P(None, "tensor"),
            P("tensor"),
            P("tensor", None),
            P(),
        ),
        check_vma=False,
    )
```
